256 devices in a mesh: image: 16 (over z, core), dp: 16 (over y, x).
Axes of the slice: x: 4, y: 4, z: 8, core: 2. Of those that a mesh axis runs over, the one named last changes fastest.
Arguments:
- features: bfloat16 [16, 128, 128, 384], P('dp', 'image'), may hold values from -6 to 6
- conv_weight: bfloat16 [3, 3, 128, 128], replicated, may hold values from -0.1875 to 0.1875
- reduce_weight: bfloat16 [256, 128], replicated, may hold values from -0.375 to 0.375
- spectral_weight: bfloat16 [256, 256], replicated, may hold values from -0.375 to 0.375
- expand_weight: bfloat16 [128, 256], replicated, may hold values from -0.5 to 0.5
- upstream: bfloat16 [16, 128, 128, 384], P('dp', 'image'), may hold values from -6 to 6
Outputs:
- feature_grad: bfloat16 [16, 128, 128, 384], P('dp', 'image')
- conv_grad: float32 [3, 3, 128, 128], replicated
- reduce_grad: float32 [256, 128], replicated
- spectral_grad: float32 [256, 256], replicated
- expand_grad: float32 [128, 256], replicated
The draws below stay inside these ranges and needn't reach their ends.
All inputs are finite; a program needn't handle non-finite values.
Results may differ from the reference program's by a relative error of at most 0.014.
Values may be sent and summed in bfloat16 or wider, within the bound.
No kernel may reach another device: no remote copies, remote signals or barrier semaphores. Data moves between devices by JAX's collectives and lax.ppermute only.
A program may use at most 64 MiB of HBM per device.

```python
import math
import jax
import jax.numpy as jnp
from jax import lax

H = 128
W = 128
CL = 128
CG = 256
CH = 128
IMAGES = 16


def level_of(stream_key, dims, cuts, least, high):
    def one(position, blocks):
        heights = jax.random.uniform(jax.random.fold_in(jax.random.fold_in(stream_key, 6), position), (blocks,), jnp.float32, least / len(cuts), high / len(cuts))
        return jnp.repeat(jnp.exp(heights), dims[position] // blocks).reshape((-1,) + (1,) * (len(dims) - position - 1))

    loudness = one(*cuts[0])
    for cut in cuts[1:]:
        loudness = loudness * one(*cut)
    return loudness


def scatter_about(stream_key, shape, width, reach, split=(), held_as=jnp.bfloat16):
    values = width * jax.random.normal(stream_key, shape, jnp.float32)
    if split:
        values = values * level_of(stream_key, shape, split, -0.22, 0.18)
    return jnp.clip(values, -reach, reach).astype(held_as)


def setup_inputs(seed: int = 0) -> dict:
    seeds = jax.random.split(jax.random.key(seed), 7)
    features = scatter_about(seeds[0], (IMAGES, H, W, CL + CG), 1.0, 6.0, ((0, 16), (1, 16)))
    conv_weight = scatter_about(seeds[1], (3, 3, CL, CL), (9 * CL) ** -0.5, 0.1875)
    reduce_weight = scatter_about(seeds[2], (CG, CH), CG ** -0.5, 0.375)
    spectral_weight = scatter_about(seeds[3], (2 * CH, 2 * CH), (2 * CH) ** -0.5, 0.375)
    expand_weight = scatter_about(seeds[4], (CH, CG), CH ** -0.5, 0.5)
    upstream = scatter_about(seeds[5], (IMAGES, H, W, CL + CG), 1.0, 6.0, ((0, 16), (1, 16)))
    return {"features": features, "conv_weight": conv_weight, "reduce_weight": reduce_weight, "spectral_weight": spectral_weight, "expand_weight": expand_weight, "upstream": upstream}


def make_tables(length, number):
    lead = lax.broadcasted_iota(jnp.int32, (length, number), 0)
    trail = lax.broadcasted_iota(jnp.int32, (length, number), 1)
    angles = (lead * trail % length).astype(jnp.float32) * (2.0 * math.pi / length)
    factor = 1.0 / math.sqrt(length)
    return ((jnp.cos(angles) * factor).astype(jnp.bfloat16), (-jnp.sin(angles) * factor).astype(jnp.bfloat16))

def inverse_tables(cosine, sine):
    number = cosine.shape[1]
    doubling = jnp.where(lax.broadcasted_iota(jnp.int32, (1, number), 1) == 0, 1.0, 2.0).astype(jnp.bfloat16)
    return ((cosine * doubling).T, (sine * doubling).T)

def product(form, left, right):
    return jnp.einsum(form, left.astype(jnp.float32), right.astype(jnp.float32))

def halves(spectrum):
    half = spectrum.shape[-1] // 2
    return (spectrum[..., :half], spectrum[..., half:])

def height_forward(spectrum, cosine, sine):
    real_part, imag_part = halves(spectrum)
    out_real = product('hm,hkc->mkc', cosine, real_part) - product('hm,hkc->mkc', sine, imag_part)
    out_imag = product('hm,hkc->mkc', cosine, imag_part) + product('hm,hkc->mkc', sine, real_part)
    return jnp.concatenate([out_real, out_imag], axis=-1)

def height_inverse(spectrum, cosine, sine):
    real_part, imag_part = halves(spectrum)
    out_real = product('hm,mkc->hkc', cosine, real_part) + product('hm,mkc->hkc', sine, imag_part)
    out_imag = product('hm,mkc->hkc', cosine, imag_part) - product('hm,mkc->hkc', sine, real_part)
    return jnp.concatenate([out_real, out_imag], axis=-1)

def width_forward(hidden, cosine, sine):
    return jnp.concatenate([product('hwc,wk->hkc', hidden, cosine), product('hwc,wk->hkc', hidden, sine)], axis=-1)

def width_forward_transpose(spectrum, cosine, sine):
    real_part, imag_part = halves(spectrum)
    return product('hkc,wk->hwc', real_part, cosine) + product('hkc,wk->hwc', imag_part, sine)

def width_inverse(spectrum, back_cos, back_sin):
    real_part, imag_part = halves(spectrum)
    return product('hkc,kw->hwc', real_part, back_cos) + product('hkc,kw->hwc', imag_part, back_sin)

def width_inverse_transpose(grad_map, back_cos, back_sin):
    return jnp.concatenate([product('hwc,kw->hkc', grad_map, back_cos), product('hwc,kw->hkc', grad_map, back_sin)], axis=-1)

def silu_slope(values):
    sigma = jax.nn.sigmoid(values)
    return sigma * (1.0 + values * (1.0 - sigma))

def conv_taps(padded, weights, row_count, col_count):
    summed = jnp.zeros((row_count * col_count, weights.shape[3]), jnp.float32)
    for tap_row in range(3):
        for tap_col in range(3):
            window = padded[tap_row:tap_row + row_count, tap_col:tap_col + col_count].reshape(row_count * col_count, -1)
            summed = summed + jnp.dot(window, weights[tap_row, tap_col], preferred_element_type=jnp.float32)
    return summed

def conv_back(padded, weights, row_count, col_count):
    summed = jnp.zeros((row_count * col_count, weights.shape[2]), jnp.float32)
    for tap_row in range(3):
        for tap_col in range(3):
            window = padded[2 - tap_row:2 - tap_row + row_count, 2 - tap_col:2 - tap_col + col_count].reshape(row_count * col_count, -1)
            summed = summed + jnp.dot(window, weights[tap_row, tap_col].T, preferred_element_type=jnp.float32)
    return summed

def conv_grad_terms(padded, grad_flat, row_count, col_count):
    taps = []
    for tap_row in range(3):
        line = []
        for tap_col in range(3):
            window = padded[tap_row:tap_row + row_count, tap_col:tap_col + col_count].reshape(row_count * col_count, -1)
            line.append(product('pi,po->io', window, grad_flat))
        taps.append(jnp.stack(line))
    return jnp.stack(taps)

def single(picture, incoming, conv_weight, reduce_weight, spectral_weight, expand_weight):
    height, breadth, channels = picture.shape
    local_count = conv_weight.shape[2]
    global_count, hidden_count = reduce_weight.shape
    frequencies = breadth // 2
    cos_width, sin_width = make_tables(breadth, frequencies)
    cos_height, sin_height = make_tables(height, height)
    back_cos, back_sin = inverse_tables(cos_width, sin_width)
    x_local = picture[..., :local_count]
    x_global = picture[..., local_count:].reshape(-1, global_count)
    local_pad = jnp.pad(x_local, ((1, 1), (1, 1), (0, 0)))
    y_local = conv_taps(local_pad, conv_weight, height, breadth)
    pre_reduce = jnp.dot(x_global, reduce_weight, preferred_element_type=jnp.float32).reshape(height, breadth, hidden_count)
    hidden = jax.nn.silu(pre_reduce).astype(jnp.bfloat16)
    spectrum = width_forward(hidden, cos_width, sin_width).astype(jnp.bfloat16)
    column_spec = height_forward(spectrum, cos_height, sin_height).astype(jnp.bfloat16)
    flat_spec = column_spec.reshape(-1, 2 * hidden_count)
    pre_mix = jnp.dot(flat_spec, spectral_weight, preferred_element_type=jnp.float32)
    mixture = jax.nn.silu(pre_mix).astype(jnp.bfloat16).reshape(column_spec.shape)
    returned = height_inverse(mixture, cos_height, sin_height).astype(jnp.bfloat16)
    spatial = width_inverse(returned, back_cos, back_sin)
    combined = (hidden.astype(jnp.float32) + spatial).astype(jnp.bfloat16).reshape(-1, hidden_count)
    y_global = jnp.dot(combined, expand_weight, preferred_element_type=jnp.float32)
    y_all = jnp.concatenate([y_local, y_global], axis=-1)
    incoming_flat = incoming.reshape(-1, channels).astype(jnp.float32)
    d_pre = (incoming_flat * silu_slope(y_all)).astype(jnp.bfloat16)
    d_local = d_pre[:, :local_count]
    d_global = d_pre[:, local_count:]
    grad_local = conv_grad_terms(local_pad, d_local, height, breadth)
    d_pad = jnp.pad(d_local.reshape(height, breadth, local_count), ((1, 1), (1, 1), (0, 0)))
    dx_local = conv_back(d_pad, conv_weight, height, breadth)
    d_combined = jnp.dot(d_global, expand_weight.T, preferred_element_type=jnp.float32).astype(jnp.bfloat16)
    grad_expand = product('pi,po->io', combined, d_global)
    d_returned = width_inverse_transpose(d_combined.reshape(height, breadth, hidden_count), back_cos, back_sin).astype(jnp.bfloat16)
    d_mixture = height_forward(d_returned, cos_height, sin_height)
    d_mix = (d_mixture.reshape(-1, 2 * hidden_count) * silu_slope(pre_mix)).astype(jnp.bfloat16)
    grad_spectral = product('pi,po->io', flat_spec, d_mix)
    d_column = jnp.dot(d_mix, spectral_weight.T, preferred_element_type=jnp.float32).astype(jnp.bfloat16).reshape(column_spec.shape)
    d_spectrum = height_inverse(d_column, cos_height, sin_height).astype(jnp.bfloat16)
    d_hidden = d_combined.reshape(height, breadth, hidden_count).astype(jnp.float32) + width_forward_transpose(d_spectrum, cos_width, sin_width)
    d_reduce = (d_hidden * silu_slope(pre_reduce)).astype(jnp.bfloat16).reshape(-1, hidden_count)
    grad_reduce = product('pi,po->io', x_global, d_reduce)
    dx_global = jnp.dot(d_reduce, reduce_weight.T, preferred_element_type=jnp.float32)
    feature_grad = (incoming_flat + jnp.concatenate([dx_local, dx_global], axis=-1)).astype(jnp.bfloat16)
    return (feature_grad.reshape(height, breadth, channels), grad_local, grad_reduce, grad_spectral, grad_expand)

def reference(features, conv_weight, reduce_weight, spectral_weight, expand_weight, upstream):

    def one_image(pair):
        return single(pair[0], pair[1], conv_weight, reduce_weight, spectral_weight, expand_weight)
    feature_grad, grad_local, grad_reduce, grad_spectral, grad_expand = lax.map(one_image, (features, upstream))
    factor = 1.0 / math.sqrt(IMAGES * H * W)
    return (feature_grad, lax.optimization_barrier(jnp.sum(grad_local, axis=0)) * factor, lax.optimization_barrier(jnp.sum(grad_reduce, axis=0)) * factor, lax.optimization_barrier(jnp.sum(grad_spectral, axis=0)) * factor, lax.optimization_barrier(jnp.sum(grad_expand, axis=0)) * factor)
```

```python
import math

import jax
import jax.numpy as jnp
import numpy as np
from jax import lax
from jax.experimental import pallas as pl
from jax.experimental.pallas import tpu as pltpu
from jax.sharding import PartitionSpec as P

BF = jnp.bfloat16
F32 = jnp.float32
PEERS = 16
ROWS = 8
BREADTH = 128
CELLS = ROWS * BREADTH
LANES = 128
OWNED = 4
HALF = ROWS // 2


def width_table():
    w = np.arange(BREADTH)
    freq = np.arange(PEERS * OWNED).reshape(PEERS, OWNED)
    phase = (w[None, None, :] * freq[:, :, None] % BREADTH) * (2.0 * math.pi / BREADTH)
    factor = 1.0 / math.sqrt(BREADTH)
    base = np.stack([np.cos(phase) * factor, -np.sin(phase) * factor], axis=2)
    table = np.einsum("jkrw,hg->kjhrgw", base, np.eye(HALF))
    return table.reshape(OWNED * PEERS * HALF * 2, HALF * BREADTH).astype(BF)


def height_table():
    height = PEERS * ROWS
    h = np.arange(height)
    phase = (h[:, None] * h[None, :] % height) * (2.0 * math.pi / height)
    factor = 1.0 / math.sqrt(height)
    cosine, sine = np.cos(phase) * factor, -np.sin(phase) * factor
    table = np.zeros((2, height, height, 2))
    table[0, :, :, 0] = cosine.T
    table[0, :, :, 1] = -sine.T
    table[1, :, :, 1] = cosine.T
    table[1, :, :, 0] = sine.T
    return table.reshape(2 * height, 2 * height).astype(BF)


def dot(left, right):
    return jnp.dot(left, right, preferred_element_type=F32)


def dot_t(left, right):
    return lax.dot_general(left, right, (((1,), (1,)), ((), ())), preferred_element_type=F32)


def slope_of(values, sigma):
    return sigma * (1.0 + values * (1.0 - sigma))


def to_owners(cells, table):
    side = jnp.concatenate([cells[: CELLS // 2], cells[CELLS // 2 :]], axis=1)
    found = dot(table, side)
    parts = [
        found[:, q * LANES : (q + 1) * LANES].reshape(OWNED, PEERS, ROWS, LANES) for q in range(2)
    ]
    joined = jnp.concatenate(parts, axis=2).astype(BF)
    return [joined[k] for k in range(OWNED)]


def from_owners(strip, table_t):
    wide = strip.astype(F32)
    halves = []
    for q in range(2):
        piece = wide[:, q * ROWS : (q + 1) * ROWS, :]
        rows = [
            piece[:, :, k * LANES : (k + 1) * LANES].reshape(PEERS * ROWS, LANES)
            for k in range(OWNED)
        ]
        halves.append(jnp.concatenate(rows, axis=0).astype(BF))
    found = dot(table_t, jnp.concatenate(halves, axis=1))
    return jnp.concatenate([found[:, :LANES], found[:, LANES:]], axis=0)


def by_frequency(columns):
    height = columns.shape[0] // 2
    return jnp.concatenate(
        [
            jnp.concatenate(
                [
                    columns[:height, k * LANES : (k + 1) * LANES],
                    columns[height:, k * LANES : (k + 1) * LANES],
                ],
                axis=1,
            )
            for k in range(OWNED)
        ],
        axis=0,
    )


def by_part(mixed):
    height = mixed.shape[0] // OWNED
    return jnp.concatenate(
        [
            jnp.concatenate(
                [
                    mixed[k * height : (k + 1) * height, r * LANES : (r + 1) * LANES]
                    for k in range(OWNED)
                ],
                axis=1,
            )
            for r in range(2)
        ],
        axis=0,
    )


def doubling():
    lane = lax.broadcasted_iota(jnp.int32, (1, OWNED * LANES), 1)
    return jnp.where((lane < LANES) & (lax.axis_index("image") == 0), 1.0, 2.0)


def forward_rows(x, u, weight, table, spec, hidden, slope, first, last):
    pre = dot(x[:, LANES:], weight[...])
    sigma = jax.nn.sigmoid(pre)
    low = (pre * sigma).astype(BF)
    hidden[...] = low
    for k, block in enumerate(to_owners(low, table[...])):
        spec[:, :, k * LANES : (k + 1) * LANES] = block
    slope[...] = slope_of(pre, sigma)
    first[: 2 * BREADTH] = x[: 2 * BREADTH, :LANES]
    first[2 * BREADTH :] = u[:BREADTH, :LANES]
    last[: 2 * BREADTH] = x[CELLS - 2 * BREADTH :, :LANES]
    last[2 * BREADTH :] = u[CELLS - BREADTH :, :LANES]


def local_part(x, u, above, below, weight, grad, terms):
    rows = jnp.concatenate([above[: 2 * BREADTH], x[:, :LANES], below[: 2 * BREADTH]], axis=0)

    def beside(cells):
        wide = cells.astype(F32)
        count = wide.shape[0]
        column = lax.broadcasted_iota(jnp.int32, wide.shape, 0) % BREADTH
        before = jnp.where(column == 0, 0.0, pltpu.roll(wide, 1, 0)).astype(BF)
        after = jnp.where(column == BREADTH - 1, 0.0, pltpu.roll(wide, count - 1, 0)).astype(BF)
        return before, after

    before, after = beside(rows)
    x3 = jnp.concatenate([before, rows, after], axis=1)
    y = jnp.zeros((CELLS + 2 * BREADTH, LANES), F32)
    for a in range(3):
        y = y + dot(
            x3[a * BREADTH : a * BREADTH + CELLS + 2 * BREADTH],
            weight[a * 3 * LANES : (a + 1) * 3 * LANES],
        )
    incoming = jnp.concatenate([above[2 * BREADTH :], u[:, :LANES], below[2 * BREADTH :]], axis=0)
    d = (incoming.astype(F32) * slope_of(y, jax.nn.sigmoid(y))).astype(BF)
    before, after = beside(d)
    d3 = jnp.concatenate([after, d, before], axis=1)
    dx = u[:, :LANES].astype(F32)
    for a in range(3):
        taps = [weight[(3 * a + b) * LANES : (3 * a + b + 1) * LANES] for b in range(3)]
        dx = dx + dot_t(
            d3[(2 - a) * BREADTH : (2 - a) * BREADTH + CELLS], jnp.concatenate(taps, axis=1)
        )
    grad[...] = dx.astype(BF)
    d_t = d[BREADTH : BREADTH + CELLS].T
    for a in range(3):
        found = dot(d_t, x3[(a + 1) * BREADTH : (a + 1) * BREADTH + CELLS])
        terms[a * 3 * LANES : (a + 1) * 3 * LANES] = found.T.astype(BF)


def columns_forward(arrived, table, table_t, weight, sent, flat, slope):
    columns = arrived[...].reshape(PEERS * ROWS * 2, OWNED * LANES)
    spec = by_frequency(dot(table[...], columns).astype(BF))
    flat[...] = spec
    pre = dot(spec, weight[...])
    sigma = jax.nn.sigmoid(pre)
    back = dot(table_t[...], by_part((pre * sigma).astype(BF)))
    sent[...] = (back * doubling()).astype(BF).reshape(sent.shape)
    slope[...] = slope_of(pre, sigma)


def middle_rows(arrived, hidden, u, weight, table, table_t, *outs):
    sent, d_combined, combined, d_global = outs
    spatial = from_owners(arrived[...], table_t[...])
    mix = (hidden[...].astype(F32) + spatial).astype(BF)
    combined[...] = mix
    y = dot(mix, weight[...])
    incoming = u[:, LANES:].astype(F32)
    d = (incoming * slope_of(y, jax.nn.sigmoid(y))).astype(BF)
    d_global[...] = d
    back = dot_t(d, weight[...]).astype(BF)
    d_combined[...] = back
    for k, block in enumerate(to_owners(back, table[...])):
        sent[:, :, k * LANES : (k + 1) * LANES] = block


def columns_backward(arrived, table, table_t, weight, slope, sent, d_mix):
    columns = arrived[...].reshape(PEERS * ROWS * 2, OWNED * LANES)
    found = by_frequency(dot(table[...], columns) * doubling())
    d = (found * slope[...]).astype(BF)
    d_mix[...] = d
    back = dot(table_t[...], by_part(dot_t(d, weight[...]).astype(BF)))
    sent[...] = back.astype(BF).reshape(sent.shape)


def last_rows(arrived, d_combined, slope, x_t, table_t, other, d_reduce, terms):
    d_hidden = d_combined[...].astype(F32) + from_owners(arrived[...], table_t[...])
    d = (d_hidden * slope[...]).astype(BF)
    d_reduce[...] = d
    terms[:, :16] = dot(x_t[...], d).astype(BF).reshape(PEERS, 16, LANES)
    terms[:, 16:] = other[...]


def transposed(x, x_t):
    x_t[...] = x[:, LANES:].T


def expand_terms(combined, d_global, terms):
    found = dot(combined[...].T, d_global[...])
    terms[...] = jnp.concatenate([found[:, :LANES], found[:, LANES:]], axis=0).astype(BF)


def spectral_terms(flat, d_mix, expand, conv, terms):
    found = dot(flat[...].T, d_mix[...])
    both = jnp.concatenate([found[:, :LANES], found[:, LANES:]], axis=0).astype(BF)
    terms[:, :32] = both.reshape(PEERS, 32, LANES)
    terms[:, 32:48] = expand[...].reshape(PEERS, 16, LANES)
    terms[:, 48:] = conv[...].reshape(PEERS, 72, LANES)


def global_grad(d_reduce, weight, u, local, out):
    out[:, :LANES] = local[...]
    out[:, LANES:] = (u[:, LANES:].astype(F32) + dot_t(d_reduce[...], weight[...])).astype(BF)


def summed(arrived, sent):
    total = jnp.sum(arrived[...].astype(F32), axis=0).astype(BF)
    sent[...] = jnp.broadcast_to(total[None], sent.shape)


def unpacked(factor, arrived, conv, reduce, spectral, expand):
    found = arrived[...].astype(F32) * factor
    reduce[...] = found[:, :16].reshape(256, LANES)
    both = found[:, 16:48].reshape(512, LANES)
    spectral[:, :LANES] = both[:256]
    spectral[:, LANES:] = both[256:]
    both = found[:, 48:64].reshape(256, LANES)
    expand[:, :LANES] = both[:128]
    expand[:, LANES:] = both[128:]
    conv[...] = found[:, 64:].reshape(9 * LANES, LANES)


WHOLE = pl.BlockSpec(memory_space=pltpu.VMEM)


def run(body, outs, *args, name=None, cost=4):
    many = isinstance(outs[0][0], tuple)
    return pl.pallas_call(
        body,
        out_shape=tuple(jax.ShapeDtypeStruct(*o) for o in outs)
        if many
        else jax.ShapeDtypeStruct(*outs),
        in_specs=[WHOLE] * len(args),
        out_specs=(WHOLE,) * len(outs) if many else WHOLE,
        name=name,
        cost_estimate=pl.CostEstimate(
            flops=int(cost * 1e8), bytes_accessed=1 << 20, transcendentals=0
        ),
        compiler_params=pltpu.CompilerParams(vmem_limit_bytes=24 << 20),
    )(*args)


def exchange(array, axis):
    return lax.all_to_all(array, axis, 0, 0, tiled=True)


def shards(features, conv_weight, reduce_weight, spectral_weight, expand_weight, upstream):
    x = features.reshape(CELLS, 3 * LANES)
    u = upstream.reshape(CELLS, 3 * LANES)
    conv = conv_weight.reshape(9 * LANES, LANES)
    width = width_table()
    height = height_table()
    wide, wide_t = jnp.asarray(width), jnp.asarray(np.ascontiguousarray(width.T))
    tall, tall_t = jnp.asarray(height), jnp.asarray(np.ascontiguousarray(height.T))
    message = ((PEERS, 2 * ROWS, OWNED * LANES), BF)
    cells = ((CELLS, LANES), BF)
    edge = ((3 * BREADTH, LANES), BF)

    spec, hidden, slope, first, last = run(
        forward_rows,
        (message, cells, ((CELLS, LANES), F32), edge, edge),
        *(x, u, reduce_weight, wide),
        name="forward_rows",
    )
    arrived = exchange(spec, "image")
    forward = [(i, i + 1) for i in range(PEERS - 1)]
    backward = [(b, a) for a, b in forward]
    above = lax.ppermute(last, "image", forward)
    below = lax.ppermute(first, "image", backward)
    local, conv_terms = run(
        local_part,
        (cells, ((9 * LANES, LANES), BF)),
        *(x, u, above, below, conv),
        name="local_part",
        cost=30,
    )
    sent, flat, mix_slope = run(
        columns_forward,
        (message, ((512, 256), BF), ((512, 256), F32)),
        *(arrived, tall, tall_t, spectral_weight),
        name="columns_forward",
    )
    arrived = exchange(sent, "image")
    x_t = run(
        transposed,
        ((256, CELLS), BF),
        x,
        name="transposed",
        cost=10,
    )
    sent, d_combined, combined, d_global = run(
        middle_rows,
        (message, cells, cells, ((CELLS, 256), BF)),
        *(arrived, hidden, u, expand_weight, wide, wide_t),
        name="middle_rows",
    )
    arrived = exchange(sent, "image")
    expand = run(expand_terms, ((256, LANES), BF), combined, d_global, name="expand_terms", cost=10)
    sent, d_mix = run(
        columns_backward,
        (message, ((512, 256), BF)),
        *(arrived, tall, tall_t, spectral_weight, mix_slope),
        name="columns_backward",
    )
    arrived = exchange(sent, "image")
    other = run(
        spectral_terms,
        ((PEERS, 120, LANES), BF),
        *(flat, d_mix, expand, conv_terms),
        name="spectral_terms",
        cost=10,
    )
    packed = ((PEERS, 136, LANES), BF)
    d_reduce, terms = run(
        last_rows,
        (cells, packed),
        *(arrived, d_combined, slope, x_t, wide_t, other),
        name="last_rows",
    )
    arrived = exchange(terms, "dp")
    grad = run(
        global_grad,
        ((CELLS, 3 * LANES), BF),
        *(d_reduce, reduce_weight, u, local),
        name="global_grad",
        cost=10,
    )
    arrived = exchange(run(summed, packed, arrived, name="sum_images"), "image")
    arrived = exchange(run(summed, packed, arrived, name="sum_strips"), "dp")
    factor = 1.0 / math.sqrt(PEERS * PEERS * ROWS * BREADTH)
    conv_sum, reduce_sum, spectral_sum, expand_sum = run(
        lambda *refs: unpacked(factor, *refs),
        (
            ((9 * LANES, LANES), F32),
            ((256, LANES), F32),
            ((256, 256), F32),
            ((128, 256), F32),
        ),
        arrived,
        name="unpacked",
    )
    return (
        grad.reshape(1, ROWS, BREADTH, 3 * LANES),
        conv_sum.reshape(3, 3, LANES, LANES),
        reduce_sum,
        spectral_sum,
        expand_sum,
    )


def solution(mesh):
    return jax.shard_map(
        shards,
        mesh=mesh,
        in_specs=(P("dp", "image", None, None), P(), P(), P(), P(), P("dp", "image", None, None)),
        out_specs=(P("dp", "image", None, None), P(), P(), P(), P()),
        check_vma=False,
    )
```

```python
import math

import jax
import jax.numpy as jnp
import numpy as np
from jax import lax
from jax.experimental import pallas as pl
from jax.experimental.pallas import tpu as pltpu
from jax.sharding import Mesh
from jax.sharding import PartitionSpec as P

BF = jnp.bfloat16
F32 = jnp.float32
PEERS = 16
ROWS = 8
BREADTH = 128
CELLS = ROWS * BREADTH
LANES = 128
OWNED = 4
HALF = ROWS // 2
MESSAGE = OWNED * 2 * ROWS
SIDE = 4
PIECE = 80
SHARE = PIECE // PEERS


def width_table():
    w = np.arange(BREADTH)
    freq = np.arange(PEERS * OWNED).reshape(PEERS, OWNED)
    phase = (w[None, None, :] * freq[:, :, None] % BREADTH) * (2.0 * math.pi / BREADTH)
    factor = 1.0 / math.sqrt(BREADTH)
    base = np.stack([np.cos(phase) * factor, -np.sin(phase) * factor], axis=2)
    table = np.einsum("jkrw,hg->kjhrgw", base, np.eye(HALF))
    return table.reshape(OWNED * PEERS * HALF * 2, HALF * BREADTH).astype(BF)


def narrow_table():
    table = width_table().reshape(OWNED, PEERS, HALF, 2, HALF, BREADTH)
    return np.einsum("kjhrhw->kjhrw", table).reshape(-1, BREADTH)


def spreading():
    table = np.zeros((PEERS, 8, PEERS, SHARE))
    for p in range(PEERS):
        for r in range(SHARE):
            table[p, r, p, r] = 1.0
    return table.reshape(PEERS * 8, PIECE).astype(BF)


def height_table():
    height = PEERS * ROWS
    h = np.arange(height)
    phase = (h[:, None] * h[None, :] % height) * (2.0 * math.pi / height)
    factor = 1.0 / math.sqrt(height)
    cosine, sine = np.cos(phase) * factor, -np.sin(phase) * factor
    table = np.zeros((2, height, height, 2))
    table[0, :, :, 0] = cosine.T
    table[0, :, :, 1] = -sine.T
    table[1, :, :, 1] = cosine.T
    table[1, :, :, 0] = sine.T
    return table.reshape(2 * height, 2 * height).astype(BF)


def dot(left, right):
    return jnp.dot(left, right, preferred_element_type=F32)


def dot_t(left, right):
    return lax.dot_general(left, right, (((1,), (1,)), ((), ())), preferred_element_type=F32)


def slope_of(values, sigma):
    return sigma * (1.0 + values * (1.0 - sigma))


def to_owners(cells, table):
    side = jnp.concatenate([cells[: CELLS // 2], cells[CELLS // 2 :]], axis=1)
    found = dot(table, side)
    parts = [
        found[:, q * LANES : (q + 1) * LANES].reshape(OWNED, PEERS, ROWS, LANES) for q in range(2)
    ]
    joined = jnp.concatenate(parts, axis=2).astype(BF)
    return [joined[k] for k in range(OWNED)]


def from_owners(strip, table_t):
    wide = strip.astype(F32)
    halves = []
    for q in range(2):
        rows = [
            wide[:, (2 * k + q) * ROWS : (2 * k + q + 1) * ROWS].reshape(PEERS * ROWS, LANES)
            for k in range(OWNED)
        ]
        halves.append(jnp.concatenate(rows, axis=0).astype(BF))
    found = dot(table_t, jnp.concatenate(halves, axis=1))
    return jnp.concatenate([found[:, :LANES], found[:, LANES:]], axis=0)


def store_message(sent, blocks):
    for k, block in enumerate(blocks):
        sent[:, 2 * k * ROWS : 2 * (k + 1) * ROWS] = block


def columns_of(arrived):
    return jnp.concatenate(
        [
            arrived[:, 2 * k * ROWS : 2 * (k + 1) * ROWS].reshape(PEERS * ROWS * 2, LANES)
            for k in range(OWNED)
        ],
        axis=1,
    )


def blocks_of(columns):
    return [
        columns[:, k * LANES : (k + 1) * LANES].reshape(PEERS, 2 * ROWS, LANES)
        for k in range(OWNED)
    ]


def by_frequency(columns):
    height = columns.shape[0] // 2
    return jnp.concatenate(
        [
            jnp.concatenate(
                [
                    columns[:height, k * LANES : (k + 1) * LANES],
                    columns[height:, k * LANES : (k + 1) * LANES],
                ],
                axis=1,
            )
            for k in range(OWNED)
        ],
        axis=0,
    )


def by_part(mixed):
    height = mixed.shape[0] // OWNED
    return jnp.concatenate(
        [
            jnp.concatenate(
                [
                    mixed[k * height : (k + 1) * height, r * LANES : (r + 1) * LANES]
                    for k in range(OWNED)
                ],
                axis=1,
            )
            for r in range(2)
        ],
        axis=0,
    )


def doubling():
    lane = lax.broadcasted_iota(jnp.int32, (1, OWNED * LANES), 1)
    return jnp.where((lane < LANES) & (lax.axis_index("image") == 0), 1.0, 2.0)


def forward_rows(x, u, weight, narrow, spec, hidden, slope, first, last, held, sems):
    inner, two = 2 * BREADTH, CELLS - 2 * BREADTH
    copies = [
        pltpu.make_async_copy(source, target, sems.at[i])
        for i, (source, target) in enumerate(
            (
                (x.at[:, pl.ds(LANES, 2 * LANES)], held),
                (x.at[pl.ds(0, inner), pl.ds(0, LANES)], first.at[pl.ds(0, inner)]),
                (x.at[pl.ds(two, inner), pl.ds(0, LANES)], last.at[pl.ds(0, inner)]),
                (u.at[pl.ds(0, BREADTH), pl.ds(0, LANES)], first.at[pl.ds(inner, BREADTH)]),
                (
                    u.at[pl.ds(CELLS - BREADTH, BREADTH), pl.ds(0, LANES)],
                    last.at[pl.ds(inner, BREADTH)],
                ),
            )
        )
    ]
    for copy in copies:
        copy.start()
    row = lax.broadcasted_iota(jnp.int32, (PEERS * OWNED * ROWS, BREADTH), 0) // 2 % HALF
    base = narrow[...]
    table = jnp.concatenate(
        [base * (row == g).astype(F32).astype(BF) for g in range(HALF)], axis=1
    )
    copies[0].wait()
    pre = dot(held[...], weight[...])
    sigma = jax.nn.sigmoid(pre)
    low = (pre * sigma).astype(BF)
    hidden[...] = low
    store_message(spec, to_owners(low, table))
    slope[...] = slope_of(pre, sigma)
    for copy in copies[1:]:
        copy.wait()


def local_part(x, u, above, below, weight, grad, own, *rest):
    sends, terms = rest[:3], rest[3]
    rows = jnp.concatenate([above[: 2 * BREADTH], x[:, :LANES], below[: 2 * BREADTH]], axis=0)

    def beside(cells):
        wide = cells.astype(F32)
        count = wide.shape[0]
        column = lax.broadcasted_iota(jnp.int32, wide.shape, 0) % BREADTH
        before = jnp.where(column == 0, 0.0, pltpu.roll(wide, 1, 0)).astype(BF)
        after = jnp.where(column == BREADTH - 1, 0.0, pltpu.roll(wide, count - 1, 0)).astype(BF)
        return before, after

    before, after = beside(rows)
    x3 = jnp.concatenate([before, rows, after], axis=1)
    y = jnp.zeros((CELLS + 2 * BREADTH, LANES), F32)
    for a in range(3):
        y = y + dot(
            x3[a * BREADTH : a * BREADTH + CELLS + 2 * BREADTH],
            weight[a * 3 * LANES : (a + 1) * 3 * LANES],
        )
    incoming = jnp.concatenate([above[2 * BREADTH :], u[:, :LANES], below[2 * BREADTH :]], axis=0)
    d = (incoming.astype(F32) * slope_of(y, jax.nn.sigmoid(y))).astype(BF)
    before, after = beside(d)
    d3 = jnp.concatenate([after, d, before], axis=1)
    dx = u[:, :LANES].astype(F32)
    for a in range(3):
        taps = [weight[(3 * a + b) * LANES : (3 * a + b + 1) * LANES] for b in range(3)]
        dx = dx + dot_t(
            d3[(2 - a) * BREADTH : (2 - a) * BREADTH + CELLS], jnp.concatenate(taps, axis=1)
        )
    grad[...] = dx.astype(BF)
    d_t = d[BREADTH : BREADTH + CELLS].T
    for a in range(3):
        found = dot(d_t, x3[(a + 1) * BREADTH : (a + 1) * BREADTH + CELLS])
        terms[a * 3 * LANES : (a + 1) * 3 * LANES] = found.T.astype(BF)
    terms[9 * LANES :] = jnp.zeros((SIDE * SIDE * PIECE - 9 * LANES, LANES), BF)
    me = lax.axis_index("x")
    for step, target in enumerate((own, *sends)):
        begin = pl.multiple_of(lax.rem(me + step, SIDE) * (SIDE * PIECE), SIDE * PIECE)
        target[...] = terms[pl.ds(begin, SIDE * PIECE)]


def sum_x(own, a, b, c, kept, *rest):
    sends, held = rest[:3], rest[3]
    total = own[...].astype(F32) + a[...].astype(F32) + b[...].astype(F32) + c[...].astype(F32)
    held[...] = total.astype(BF)
    me = lax.axis_index("y")
    for step, target in enumerate((kept, *sends)):
        begin = pl.multiple_of(lax.rem(me + step, SIDE) * PIECE, PIECE)
        target[...] = held[pl.ds(begin, PIECE)]


def join_y(own, a, b, c, whole):
    me = lax.axis_index("y")
    for step, piece in enumerate((own, a, b, c)):
        begin = pl.multiple_of(lax.rem(me - step + SIDE, SIDE) * PIECE, PIECE)
        whole[pl.ds(begin, PIECE)] = piece[...]


def columns_forward(arrived, table, table_t, weight, sent, flat, slope):
    spec = by_frequency(dot(table[...], columns_of(arrived)).astype(BF))
    flat[...] = spec
    pre = dot(spec, weight[...])
    sigma = jax.nn.sigmoid(pre)
    back = dot(table_t[...], by_part((pre * sigma).astype(BF)))
    store_message(sent, blocks_of((back * doubling()).astype(BF)))
    slope[...] = slope_of(pre, sigma)


def middle_rows(arrived, hidden, u, weight, table, table_t, spread, pa, pb, pc, pd, *outs):
    sent, d_combined, combined, d_global = outs
    total = pa[...].astype(F32) + pb[...].astype(F32) + pc[...].astype(F32) + pd[...].astype(F32)
    shares = dot(spread[...], total.astype(BF)).astype(BF)
    sent[:, MESSAGE:] = shares.reshape(PEERS, 8, LANES)
    spatial = from_owners(arrived[...], table_t[...])
    mix = (hidden[...].astype(F32) + spatial).astype(BF)
    combined[...] = mix
    y = dot(mix, weight[...])
    incoming = u[:, LANES:].astype(F32)
    d = (incoming * slope_of(y, jax.nn.sigmoid(y))).astype(BF)
    d_global[...] = d
    back = dot_t(d, weight[...]).astype(BF)
    d_combined[...] = back
    store_message(sent, to_owners(back, table[...]))


def columns_backward(arrived, table, table_t, weight, slope, sent, d_mix):
    share = jnp.sum(arrived[:, MESSAGE:].astype(F32), axis=0).astype(BF)
    sent[:, MESSAGE:] = jnp.broadcast_to(share[None], (PEERS, 8, LANES))
    found = by_frequency(dot(table[...], columns_of(arrived)) * doubling())
    d = (found * slope[...]).astype(BF)
    d_mix[...] = d
    back = dot(table_t[...], by_part(dot_t(d, weight[...]).astype(BF)))
    store_message(sent, blocks_of(back.astype(BF)))


def last_rows(arrived, d_combined, slope, x_t, table_t, spread, other, d_reduce, terms, piece):
    d_hidden = d_combined[...].astype(F32) + from_owners(arrived[:, :MESSAGE], table_t[...])
    d = (d_hidden * slope[...]).astype(BF)
    d_reduce[...] = d
    terms[:, :16] = dot(x_t[...], d).astype(BF).reshape(PEERS, 16, LANES)
    terms[:, 16:] = other[...]
    shares = arrived[:, MESSAGE:].reshape(PEERS * 8, LANES)
    found = lax.dot_general(
        spread[...], shares, (((0,), (0,)), ((), ())), preferred_element_type=F32
    )
    piece[...] = found.astype(BF)


def transposed(x, x_t):
    x_t[...] = x[:, LANES:].T


def expand_terms(combined, d_global, terms):
    found = dot(combined[...].T, d_global[...])
    terms[...] = jnp.concatenate([found[:, :LANES], found[:, LANES:]], axis=0).astype(BF)


def spectral_terms(flat, d_mix, expand, terms):
    found = dot(flat[...].T, d_mix[...])
    both = jnp.concatenate([found[:, :LANES], found[:, LANES:]], axis=0).astype(BF)
    terms[:, :32] = both.reshape(PEERS, 32, LANES)
    terms[:, 32:] = expand[...].reshape(PEERS, 16, LANES)


def global_grad(d_reduce, weight, u, local, out):
    out[:, :LANES] = local[...]
    out[:, LANES:] = (u[:, LANES:].astype(F32) + dot_t(d_reduce[...], weight[...])).astype(BF)


def summed(arrived, sent):
    total = jnp.sum(arrived[...].astype(F32), axis=0).astype(BF)
    sent[...] = jnp.broadcast_to(total[None], sent.shape)


def unpacked(factor, arrived, pa, pb, pc, pd, conv, reduce, spectral, expand, held):
    me = lax.axis_index("x")
    for step, piece in enumerate((pa, pb, pc, pd)):
        begin = pl.multiple_of(lax.rem(me - step + SIDE, SIDE) * (SIDE * PIECE), SIDE * PIECE)
        held[pl.ds(begin, SIDE * PIECE)] = piece[...]
    conv[...] = held[: 9 * LANES].astype(F32) * factor
    found = arrived[...].astype(F32) * factor
    reduce[...] = found[:, :16].reshape(256, LANES)
    both = found[:, 16:48].reshape(512, LANES)
    spectral[:, :LANES] = both[:256]
    spectral[:, LANES:] = both[256:]
    both = found[:, 48:64].reshape(256, LANES)
    expand[:, :LANES] = both[:128]
    expand[:, LANES:] = both[128:]


WHOLE = pl.BlockSpec(memory_space=pltpu.VMEM)
APART = pl.BlockSpec(memory_space=pltpu.HBM)


def placed(shape, dtype, near=True):
    return pltpu.VMEM(shape, dtype) if near else jax.ShapeDtypeStruct(shape, dtype)


def run(body, outs, *args, name=None, cost=4, specs=None, scratch=()):
    many = isinstance(outs[0][0], tuple)
    return pl.pallas_call(
        body,
        out_shape=tuple(placed(*o) for o in outs) if many else placed(*outs),
        in_specs=specs or [WHOLE] * len(args),
        out_specs=(WHOLE,) * len(outs) if many else WHOLE,
        scratch_shapes=scratch,
        name=name,
        cost_estimate=pl.CostEstimate(
            flops=int(cost * 1e8), bytes_accessed=1 << 20, transcendentals=0
        ),
        compiler_params=pltpu.CompilerParams(vmem_limit_bytes=24 << 20),
    )(*args)


def around(arrays, axis):
    return [
        lax.ppermute(a, axis, [(i, (i + d) % SIDE) for i in range(SIDE)])
        for d, a in enumerate(arrays, 1)
    ]


def exchange(array, axis):
    return lax.all_to_all(array, axis, 0, 0, tiled=True)


def shards(features, conv_weight, reduce_weight, spectral_weight, expand_weight, upstream):
    x = features.reshape(CELLS, 3 * LANES)
    u = upstream.reshape(CELLS, 3 * LANES)
    conv = conv_weight.reshape(9 * LANES, LANES)
    width = width_table()
    height = height_table()
    wide, wide_t = jnp.asarray(width), jnp.asarray(np.ascontiguousarray(width.T))
    tall, tall_t = jnp.asarray(height), jnp.asarray(np.ascontiguousarray(height.T))
    spread = jnp.asarray(spreading())
    message = ((PEERS, MESSAGE, LANES), BF)
    longer = ((PEERS, MESSAGE + 8, LANES), BF)
    cells = ((CELLS, LANES), BF)
    edge = ((3 * BREADTH, LANES), BF)
    quarter, piece = ((SIDE * PIECE, LANES), BF), ((PIECE, LANES), BF)

    spec, hidden, slope, first, last = run(
        forward_rows,
        (message, cells, ((CELLS, LANES), F32), edge, edge),
        *(pltpu.with_memory_space_constraint(a, pltpu.HBM) for a in (x, u)),
        *(reduce_weight, jnp.asarray(narrow_table())),
        specs=[APART, APART, WHOLE, WHOLE],
        scratch=(pltpu.VMEM((CELLS, 2 * LANES), BF), pltpu.SemaphoreType.DMA((5,))),
        name="forward_rows",
    )
    arrived = exchange(spec, "image")
    forward = [(i, i + 1) for i in range(PEERS - 1)]
    above = lax.ppermute(last, "image", forward)
    below = lax.ppermute(first, "image", [(b, a) for a, b in forward])
    local, own, *sends = run(
        local_part,
        (cells, *(quarter,) * 4),
        *(x, u, above, below, conv),
        scratch=(pltpu.VMEM((SIDE * SIDE * PIECE, LANES), BF),),
        name="local_part",
        cost=30,
    )
    sent, flat, mix_slope = run(
        columns_forward,
        (message, ((512, 256), BF), ((512, 256), F32)),
        *(arrived, tall, tall_t, spectral_weight),
        name="columns_forward",
    )
    sent, own, *sends = lax.optimization_barrier((sent, own, *sends))
    arrived = exchange(sent, "image")
    own, *sends = run(
        sum_x,
        (piece,) * 4,
        own,
        *around(sends, "x"),
        scratch=(pltpu.VMEM((SIDE * PIECE, LANES), BF),),
        name="sum_x",
    )
    pieces = around(sends, "y")
    sent, d_combined, combined, d_global = run(
        middle_rows,
        (longer, cells, cells, ((CELLS, 256), BF)),
        *(arrived, hidden, u, expand_weight, wide, wide_t, spread, own, *pieces),
        name="middle_rows",
    )
    arrived = exchange(sent, "image")
    expand = run(expand_terms, ((256, LANES), BF), combined, d_global, name="expand_terms", cost=10)
    x_t = run(transposed, ((256, CELLS), BF), x, name="transposed", cost=10)
    sent, d_mix = run(
        columns_backward,
        (longer, ((512, 256), BF)),
        *(arrived, tall, tall_t, spectral_weight, mix_slope),
        name="columns_backward",
    )
    arrived = exchange(sent, "image")
    other = run(
        spectral_terms,
        ((PEERS, 48, LANES), BF),
        *(flat, d_mix, expand),
        name="spectral_terms",
        cost=10,
    )
    packed = ((PEERS, 64, LANES), BF)
    d_reduce, terms, whole = run(
        last_rows,
        (cells, packed, piece),
        *(arrived, d_combined, slope, x_t, wide_t, spread, other),
        name="last_rows",
    )
    arrived = exchange(terms, ("y", "x"))
    whole = run(join_y, quarter, whole, *around([whole] * 3, "y"), name="join_y")
    sums, whole = lax.optimization_barrier(
        (run(summed, packed, arrived, name="sum_images"), whole)
    )
    arrived = exchange(sums, "image")
    pieces = around([whole] * 3, "x")
    grad = run(
        global_grad,
        ((CELLS, 3 * LANES), BF, False),
        *(d_reduce, reduce_weight, u, local),
        name="global_grad",
        cost=10,
    )
    sums, *pieces = lax.optimization_barrier(
        (run(summed, packed, arrived, name="sum_strips"), *pieces)
    )
    arrived = exchange(sums, ("y", "x"))
    factor = 1.0 / math.sqrt(PEERS * PEERS * ROWS * BREADTH)
    conv_sum, reduce_sum, spectral_sum, expand_sum = run(
        lambda *refs: unpacked(factor, *refs),
        (
            ((9 * LANES, LANES), F32, False),
            ((256, LANES), F32, False),
            ((256, 256), F32, False),
            ((128, 256), F32, False),
        ),
        *(arrived, whole, *pieces),
        scratch=(pltpu.VMEM((SIDE * SIDE * PIECE, LANES), BF),),
        name="unpacked",
    )
    return (
        grad.reshape(1, ROWS, BREADTH, 3 * LANES),
        conv_sum.reshape(3, 3, LANES, LANES),
        reduce_sum,
        spectral_sum,
        expand_sum,
    )


def solution(mesh):
    strips = P(("y", "x"), "image", None, None)
    return jax.shard_map(
        shards,
        mesh=Mesh(mesh.devices.reshape(PEERS, SIDE, SIDE), ("image", "y", "x")),
        in_specs=(strips, P(), P(), P(), P(), strips),
        out_specs=(strips, P(), P(), P(), P()),
        check_vma=False,
    )
```

```python
import math

import jax
import jax.numpy as jnp
import numpy as np
from jax import lax
from jax.experimental import pallas as pl
from jax.experimental.pallas import tpu as pltpu
from jax.sharding import Mesh
from jax.sharding import PartitionSpec as P

BF = jnp.bfloat16
F32 = jnp.float32
PEERS = 16
ROWS = 8
BREADTH = 128
CELLS = ROWS * BREADTH
LANES = 128
OWNED = 4
HALF = ROWS // 2
SIDE = 4
LEVELS = 8
IMAGE = ("z", "core")
DP = ("y", "x")
CONV = 40
TERMS = 16 + 8 + CONV + 8


def width_table():
    w = np.arange(BREADTH)
    freq = np.arange(PEERS * OWNED).reshape(PEERS, OWNED)
    phase = (w[None, None, :] * freq[:, :, None] % BREADTH) * (2.0 * math.pi / BREADTH)
    factor = 1.0 / math.sqrt(BREADTH)
    base = np.stack([np.cos(phase) * factor, -np.sin(phase) * factor], axis=2)
    table = np.einsum("jkrw,hg->kjhrgw", base, np.eye(HALF))
    return table.reshape(OWNED * PEERS * HALF * 2, HALF * BREADTH).astype(BF)


def narrow_table():
    table = width_table().reshape(OWNED, PEERS, HALF, 2, HALF, BREADTH)
    return np.einsum("kjhrhw->kjhrw", table).reshape(-1, BREADTH)


def height_table():
    height = PEERS * ROWS
    h = np.arange(height)
    phase = (h[:, None] * h[None, :] % height) * (2.0 * math.pi / height)
    factor = 1.0 / math.sqrt(height)
    cosine, sine = np.cos(phase) * factor, -np.sin(phase) * factor
    table = np.zeros((2, height, height, 2))
    table[0, :, :, 0] = cosine.T
    table[0, :, :, 1] = -sine.T
    table[1, :, :, 1] = cosine.T
    table[1, :, :, 0] = sine.T
    return table.reshape(2 * height, 2 * height).astype(BF)


def dot(left, right):
    return jnp.dot(left, right, preferred_element_type=F32)


def dot_t(left, right):
    return lax.dot_general(left, right, (((1,), (1,)), ((), ())), preferred_element_type=F32)


def slope_of(values, sigma):
    return sigma * (1.0 + values * (1.0 - sigma))


def to_owners(cells, table):
    side = jnp.concatenate([cells[: CELLS // 2], cells[CELLS // 2 :]], axis=1)
    found = dot(table, side)
    parts = [
        found[:, q * LANES : (q + 1) * LANES].reshape(OWNED, PEERS, ROWS, LANES) for q in range(2)
    ]
    joined = jnp.concatenate(parts, axis=2).astype(BF)
    return [joined[k] for k in range(OWNED)]


def from_owners(strip, table_t):
    wide = strip.astype(F32)
    halves = []
    for q in range(2):
        rows = [
            wide[:, (2 * k + q) * ROWS : (2 * k + q + 1) * ROWS].reshape(PEERS * ROWS, LANES)
            for k in range(OWNED)
        ]
        halves.append(jnp.concatenate(rows, axis=0).astype(BF))
    found = dot(table_t, jnp.concatenate(halves, axis=1))
    return jnp.concatenate([found[:, :LANES], found[:, LANES:]], axis=0)


def store_message(sent, blocks):
    for k, block in enumerate(blocks):
        sent[:, 2 * k * ROWS : 2 * (k + 1) * ROWS] = block


def columns_of(arrived):
    return jnp.concatenate(
        [
            arrived[:, 2 * k * ROWS : 2 * (k + 1) * ROWS].reshape(PEERS * ROWS * 2, LANES)
            for k in range(OWNED)
        ],
        axis=1,
    )


def blocks_of(columns):
    return [
        columns[:, k * LANES : (k + 1) * LANES].reshape(PEERS, 2 * ROWS, LANES)
        for k in range(OWNED)
    ]


def by_frequency(columns):
    height = columns.shape[0] // 2
    return jnp.concatenate(
        [
            jnp.concatenate(
                [
                    columns[:height, k * LANES : (k + 1) * LANES],
                    columns[height:, k * LANES : (k + 1) * LANES],
                ],
                axis=1,
            )
            for k in range(OWNED)
        ],
        axis=0,
    )


def by_part(mixed):
    height = mixed.shape[0] // OWNED
    return jnp.concatenate(
        [
            jnp.concatenate(
                [
                    mixed[k * height : (k + 1) * height, r * LANES : (r + 1) * LANES]
                    for k in range(OWNED)
                ],
                axis=1,
            )
            for r in range(2)
        ],
        axis=0,
    )


def doubling():
    lane = lax.broadcasted_iota(jnp.int32, (1, OWNED * LANES), 1)
    first = lax.axis_index(IMAGE) == 0
    return jnp.where((lane < LANES) & first, 1.0, 2.0)


def started(copies, sems):
    made = [pltpu.make_async_copy(a, b, sems.at[i]) for i, (a, b) in enumerate(copies)]
    for copy in made:
        copy.start()
    return made


def forward_rows(x, u, weight, narrow, spec, hidden, slope, first, last, *scratch):
    held, near_weight, base, sems = scratch
    edge, local = 2 * BREADTH, pl.ds(0, LANES)
    copies = started(
        [
            (narrow, base),
            (weight, near_weight),
            (x.at[:, pl.ds(LANES, 2 * LANES)], held),
            (x.at[pl.ds(0, edge), local], first.at[pl.ds(0, edge)]),
            (x.at[pl.ds(CELLS - edge, edge), local], last.at[pl.ds(0, edge)]),
            (u.at[pl.ds(0, BREADTH), local], first.at[pl.ds(edge, BREADTH)]),
            (u.at[pl.ds(CELLS - BREADTH, BREADTH), local], last.at[pl.ds(edge, BREADTH)]),
        ],
        sems,
    )
    copies[0].wait()
    row = lax.broadcasted_iota(jnp.int32, (PEERS * OWNED * ROWS, BREADTH), 0) // 2 % HALF
    table = jnp.concatenate(
        [base[...] * (row == g).astype(F32).astype(BF) for g in range(HALF)], axis=1
    )
    copies[1].wait()
    copies[2].wait()
    pre = dot(held[...], near_weight[...])
    sigma = jax.nn.sigmoid(pre)
    low = (pre * sigma).astype(BF)
    hidden[...] = low
    store_message(spec, to_owners(low, table))
    slope[...] = slope_of(pre, sigma)
    for copy in copies[3:]:
        copy.wait()


def local_part(far_x, far_u, above, below, far_weight, grad, terms, x, u, weight, sems):
    local = (slice(None), pl.ds(0, LANES))
    copies = started([(far_x.at[local], x), (far_u.at[local], u), (far_weight, weight)], sems)
    for copy in copies:
        copy.wait()
    rows = jnp.concatenate([above[: 2 * BREADTH], x[...], below[: 2 * BREADTH]], axis=0)

    def beside(cells):
        wide = cells.astype(F32)
        count = wide.shape[0]
        column = lax.broadcasted_iota(jnp.int32, wide.shape, 0) % BREADTH
        before = jnp.where(column == 0, 0.0, pltpu.roll(wide, 1, 0)).astype(BF)
        after = jnp.where(column == BREADTH - 1, 0.0, pltpu.roll(wide, count - 1, 0)).astype(BF)
        return before, after

    before, after = beside(rows)
    x3 = jnp.concatenate([before, rows, after], axis=1)
    y = jnp.zeros((CELLS + 2 * BREADTH, LANES), F32)
    for a in range(3):
        y = y + dot(
            x3[a * BREADTH : a * BREADTH + CELLS + 2 * BREADTH],
            weight[a * 3 * LANES : (a + 1) * 3 * LANES],
        )
    incoming = jnp.concatenate([above[2 * BREADTH :], u[...], below[2 * BREADTH :]], axis=0)
    d = (incoming.astype(F32) * slope_of(y, jax.nn.sigmoid(y))).astype(BF)
    before, after = beside(d)
    d3 = jnp.concatenate([after, d, before], axis=1)
    dx = u[...].astype(F32)
    for a in range(3):
        taps = [weight[(3 * a + b) * LANES : (3 * a + b + 1) * LANES] for b in range(3)]
        dx = dx + dot_t(
            d3[(2 - a) * BREADTH : (2 - a) * BREADTH + CELLS], jnp.concatenate(taps, axis=1)
        )
    grad[...] = dx.astype(BF)
    d_t = d[BREADTH : BREADTH + CELLS].T
    for a in range(3):
        found = dot(d_t, x3[(a + 1) * BREADTH : (a + 1) * BREADTH + CELLS])
        terms[a * 3 * LANES : (a + 1) * 3 * LANES] = found.T.astype(BF)
    terms[9 * LANES :] = jnp.zeros((2 * PEERS * CONV - 9 * LANES, LANES), BF)


def columns_forward(arrived, table, table_t, weight, sent, flat, slope):
    spec = by_frequency(dot(table[...], columns_of(arrived)).astype(BF))
    flat[...] = spec
    pre = dot(spec, weight[...])
    sigma = jax.nn.sigmoid(pre)
    back = dot(table_t[...], by_part((pre * sigma).astype(BF)))
    store_message(sent, blocks_of((back * doubling()).astype(BF)))
    slope[...] = slope_of(pre, sigma)


def middle_rows(arrived, hidden, u, weight, table, table_t, sent, d_combined, expand):
    spatial = from_owners(arrived[...], table_t[...])
    mix = (hidden[...].astype(F32) + spatial).astype(BF)
    y = dot(mix, weight[...])
    incoming = u[:, LANES:].astype(F32)
    d = (incoming * slope_of(y, jax.nn.sigmoid(y))).astype(BF)
    back = dot_t(d, weight[...]).astype(BF)
    d_combined[...] = back
    store_message(sent, to_owners(back, table[...]))
    found = dot(mix.T, d)
    expand[...] = jnp.concatenate([found[:, :LANES], found[:, LANES:]], axis=0).astype(BF)


def columns_backward(arrived, table, table_t, weight, slope, flat, expand, conv, sent, terms):
    found = by_frequency(dot(table[...], columns_of(arrived)) * doubling())
    d = (found * slope[...]).astype(BF)
    back = dot(table_t[...], by_part(dot_t(d, weight[...]).astype(BF)))
    store_message(sent, blocks_of(back.astype(BF)))
    spectral = dot(flat[...].T, d)
    for c in range(2):
        part = spectral[:, c * LANES : (c + 1) * LANES].reshape(PEERS, 16, LANES)
        terms[c, :, :16] = part.astype(BF)
        part = expand[c * LANES : (c + 1) * LANES].astype(F32).reshape(PEERS, 8, LANES)
        terms[c, :, 16:24] = part.astype(BF)
        part = conv[c * PEERS * CONV : (c + 1) * PEERS * CONV].astype(F32)
        terms[c, :, 24:] = part.reshape(PEERS, CONV, LANES).astype(BF)


def last_rows(arrived, d_combined, slope, x, table_t, other, d_reduce, kept, sent, terms):
    d_hidden = d_combined[...].astype(F32) + from_owners(arrived[...], table_t[...])
    d = (d_hidden * slope[...]).astype(BF)
    d_reduce[...] = d
    found = dot(d.T, x[:, LANES:]).T
    terms[...] = found.reshape(2, PEERS, 8, LANES).astype(BF)
    me = lax.axis_index("core")
    for target, core in ((kept, me), (sent, 1 - me)):
        target[:, : TERMS - 8] = other[core]
        target[:, TERMS - 8 :] = terms[core]


def added(kept, other, out):
    out[...] = (kept[...].astype(F32) + other[...].astype(F32)).astype(BF)


def global_grad(d_reduce, weight, u, local, out):
    out[:, :LANES] = local[...]
    out[:, LANES:] = (u[:, LANES:].astype(F32) + dot_t(d_reduce[...], weight[...])).astype(BF)


def summed(arrived, sent):
    total = jnp.sum(arrived[...].astype(F32), axis=0).astype(BF)
    sent[...] = jnp.broadcast_to(total[None], sent.shape)


def unpacked(factor, mine, other, conv, reduce, spectral, expand, held):
    me = lax.axis_index("core")
    held[me] = mine[...]
    held[1 - me] = other[...]
    for c in range(2):
        found = held[c].astype(F32) * factor
        spectral[:, c * LANES : (c + 1) * LANES] = found[:, :16].reshape(256, LANES)
        expand[:, c * LANES : (c + 1) * LANES] = found[:, 16:24].reshape(LANES, LANES)
        begin = c * PEERS * CONV
        count = min(PEERS * CONV, 9 * LANES - begin)
        part = found[:, 24 : 24 + CONV].reshape(PEERS * CONV, LANES)
        conv[begin : begin + count] = part[:count]
        reduce[c * LANES : (c + 1) * LANES] = found[:, TERMS - 8 :].reshape(LANES, LANES)


WHOLE = pl.BlockSpec(memory_space=pltpu.VMEM)
APART = pl.BlockSpec(memory_space=pltpu.HBM)


def placed(shape, dtype, near=True):
    return pltpu.VMEM(shape, dtype) if near else jax.ShapeDtypeStruct(shape, dtype)


def run(body, outs, *args, name=None, cost=4, specs=None, scratch=()):
    many = isinstance(outs[0][0], tuple)
    return pl.pallas_call(
        body,
        out_shape=tuple(placed(*o) for o in outs) if many else placed(*outs),
        in_specs=specs or [WHOLE] * len(args),
        out_specs=(WHOLE,) * len(outs) if many else WHOLE,
        scratch_shapes=scratch,
        name=name,
        cost_estimate=pl.CostEstimate(
            flops=int(cost * 1e8), bytes_accessed=1 << 20, transcendentals=0
        ),
        compiler_params=pltpu.CompilerParams(vmem_limit_bytes=24 << 20),
    )(*args)


def far(*arrays):
    return [pltpu.with_memory_space_constraint(a, pltpu.HBM) for a in arrays]


def other_core(array):
    return lax.ppermute(array, "core", [(0, 1), (1, 0)])


def exchange(array, axis):
    return lax.all_to_all(array, axis, 0, 0, tiled=True)


def shards(features, conv_weight, reduce_weight, spectral_weight, expand_weight, upstream):
    x = features.reshape(CELLS, 3 * LANES)
    u = upstream.reshape(CELLS, 3 * LANES)
    conv = conv_weight.reshape(9 * LANES, LANES)
    width = width_table()
    height = height_table()
    wide, wide_t = jnp.asarray(width), jnp.asarray(np.ascontiguousarray(width.T))
    tall, tall_t = jnp.asarray(height), jnp.asarray(np.ascontiguousarray(height.T))
    message = ((PEERS, OWNED * 2 * ROWS, LANES), BF)
    cells = ((CELLS, LANES), BF)
    edge = ((3 * BREADTH, LANES), BF)

    spec, hidden, slope, first, last = run(
        forward_rows,
        (message, cells, ((CELLS, LANES), F32), edge, edge),
        *far(x, u, reduce_weight, jnp.asarray(narrow_table())),
        specs=[APART] * 4,
        scratch=(
            pltpu.VMEM((CELLS, 2 * LANES), BF),
            pltpu.VMEM((2 * LANES, LANES), BF),
            pltpu.VMEM((OWNED * PEERS * ROWS, LANES), BF),
            pltpu.SemaphoreType.DMA((7,)),
        ),
        name="forward_rows",
    )
    arrived = exchange(spec, IMAGE)
    forward = [(i, i + 1) for i in range(PEERS - 1)]
    above = lax.ppermute(last, IMAGE, forward)
    below = lax.ppermute(first, IMAGE, [(b, a) for a, b in forward])
    local, conv_terms = run(
        local_part,
        (cells, ((2 * PEERS * CONV, LANES), BF)),
        *(*far(x, u), above, below, *far(conv)),
        specs=[APART, APART, WHOLE, WHOLE, APART],
        scratch=(
            pltpu.VMEM((CELLS, LANES), BF),
            pltpu.VMEM((CELLS, LANES), BF),
            pltpu.VMEM((9 * LANES, LANES), BF),
            pltpu.SemaphoreType.DMA((3,)),
        ),
        name="local_part",
        cost=30,
    )
    sent, flat, mix_slope = run(
        columns_forward,
        (message, ((512, 256), BF), ((512, 256), F32)),
        *(arrived, tall, tall_t, spectral_weight),
        name="columns_forward",
    )
    sent, conv_terms, local = lax.optimization_barrier((sent, conv_terms, local))
    arrived = exchange(sent, IMAGE)
    sent, d_combined, expand = run(
        middle_rows,
        (message, cells, ((2 * LANES, LANES), BF)),
        *(arrived, hidden, u, expand_weight, wide, wide_t),
        name="middle_rows",
    )
    arrived = exchange(sent, IMAGE)
    sent, other = run(
        columns_backward,
        (message, ((2, PEERS, TERMS - 8, LANES), BF)),
        *(arrived, tall, tall_t, spectral_weight, mix_slope, flat, expand, conv_terms),
        name="columns_backward",
    )
    arrived = exchange(sent, IMAGE)
    packed = ((PEERS, TERMS, LANES), BF)
    d_reduce, kept, sent = run(
        last_rows,
        (cells, packed, packed),
        *(arrived, d_combined, slope, x, wide_t, other),
        scratch=(pltpu.VMEM((2, PEERS, 8, LANES), BF),),
        name="last_rows",
    )
    arrived = other_core(sent)
    grad = run(
        global_grad,
        ((CELLS, 3 * LANES), BF, False),
        *(d_reduce, reduce_weight, u, local),
        name="global_grad",
        cost=10,
    )
    sums, grad = lax.optimization_barrier((run(added, packed, kept, arrived, name="added"), grad))
    arrived = exchange(sums, DP)
    sums = run(summed, ((LEVELS, TERMS, LANES), BF), arrived, name="sum_images")
    arrived = exchange(sums, "z")
    sums = run(summed, packed, arrived, name="sum_strips")
    arrived = exchange(sums, DP)
    factor = 1.0 / math.sqrt(PEERS * PEERS * ROWS * BREADTH)
    conv_sum, reduce_sum, spectral_sum, expand_sum = run(
        lambda *refs: unpacked(factor, *refs),
        (
            ((9 * LANES, LANES), F32, False),
            ((256, LANES), F32, False),
            ((256, 256), F32, False),
            ((128, 256), F32, False),
        ),
        *(arrived, other_core(arrived)),
        scratch=(pltpu.VMEM((2, PEERS, TERMS, LANES), BF),),
        name="unpacked",
    )
    return (
        grad.reshape(1, ROWS, BREADTH, 3 * LANES),
        conv_sum.reshape(3, 3, LANES, LANES),
        reduce_sum,
        spectral_sum,
        expand_sum,
    )


def solution(mesh):
    strips = P(DP, IMAGE, None, None)
    return jax.shard_map(
        shards,
        mesh=Mesh(mesh.devices.reshape(LEVELS, 2, SIDE, SIDE), (*IMAGE, *DP)),
        in_specs=(strips, P(), P(), P(), P(), strips),
        out_specs=(strips, P(), P(), P(), P()),
        check_vma=False,
    )
```

```python
import functools
import math

import jax
import jax.numpy as jnp
import numpy as np
from jax import lax
from jax.experimental import pallas as pl
from jax.experimental.pallas import tpu as pltpu
from jax.sharding import Mesh
from jax.sharding import PartitionSpec as P

BF = jnp.bfloat16
F32 = jnp.float32
PEERS = 16
ROWS = 8
BREADTH = 128
CELLS = ROWS * BREADTH
LANES = 128
OWNED = 4
HALF = ROWS // 2
SIDE = 4
LEVELS = 8
IMAGE = ("z", "core")
DP = ("y", "x")
CONV = 40
TERMS = 16 + 8 + CONV + 8


def width_table():
    w = np.arange(BREADTH)
    freq = np.arange(PEERS * OWNED).reshape(PEERS, OWNED)
    phase = (w[None, None, :] * freq[:, :, None] % BREADTH) * (2.0 * math.pi / BREADTH)
    factor = 1.0 / math.sqrt(BREADTH)
    base = np.stack([np.cos(phase) * factor, -np.sin(phase) * factor], axis=2)
    table = np.einsum("jkrw,hg->kjhrgw", base, np.eye(HALF))
    return table.reshape(OWNED * PEERS * HALF * 2, HALF * BREADTH).astype(BF)


def narrow_table():
    table = width_table().reshape(OWNED, PEERS, HALF, 2, HALF, BREADTH)
    return np.einsum("kjhrhw->kjhrw", table).reshape(-1, BREADTH)


def height_table():
    height = PEERS * ROWS
    h = np.arange(height)
    phase = (h[:, None] * h[None, :] % height) * (2.0 * math.pi / height)
    factor = 1.0 / math.sqrt(height)
    cosine, sine = np.cos(phase) * factor, -np.sin(phase) * factor
    table = np.zeros((2, height, height, 2))
    table[0, :, :, 0] = cosine.T
    table[0, :, :, 1] = -sine.T
    table[1, :, :, 1] = cosine.T
    table[1, :, :, 0] = sine.T
    return table.reshape(2 * height, 2 * height).astype(BF)


def dot(left, right):
    return jnp.dot(left, right, preferred_element_type=F32)


def dot_t(left, right):
    return lax.dot_general(left, right, (((1,), (1,)), ((), ())), preferred_element_type=F32)


def slope_of(values, sigma):
    return sigma * (1.0 + values * (1.0 - sigma))


def to_owners(cells, table):
    side = jnp.concatenate([cells[: CELLS // 2], cells[CELLS // 2 :]], axis=1)
    found = dot(table, side)
    parts = [
        found[:, q * LANES : (q + 1) * LANES].reshape(OWNED, PEERS, ROWS, LANES) for q in range(2)
    ]
    joined = jnp.concatenate(parts, axis=2).astype(BF)
    return [joined[k] for k in range(OWNED)]


def from_owners(strip, table_t):
    wide = strip.astype(F32)
    halves = []
    for q in range(2):
        rows = [
            wide[:, (2 * k + q) * ROWS : (2 * k + q + 1) * ROWS].reshape(PEERS * ROWS, LANES)
            for k in range(OWNED)
        ]
        halves.append(jnp.concatenate(rows, axis=0).astype(BF))
    found = dot(table_t, jnp.concatenate(halves, axis=1))
    return jnp.concatenate([found[:, :LANES], found[:, LANES:]], axis=0)


def store_message(sent, blocks):
    for k, block in enumerate(blocks):
        sent[:, 2 * k * ROWS : 2 * (k + 1) * ROWS] = block


def columns_of(arrived):
    return jnp.concatenate(
        [
            arrived[:, 2 * k * ROWS : 2 * (k + 1) * ROWS].reshape(PEERS * ROWS * 2, LANES)
            for k in range(OWNED)
        ],
        axis=1,
    )


def blocks_of(columns):
    return [
        columns[:, k * LANES : (k + 1) * LANES].reshape(PEERS, 2 * ROWS, LANES)
        for k in range(OWNED)
    ]


def by_frequency(columns):
    height = columns.shape[0] // 2
    return jnp.concatenate(
        [
            jnp.concatenate(
                [
                    columns[:height, k * LANES : (k + 1) * LANES],
                    columns[height:, k * LANES : (k + 1) * LANES],
                ],
                axis=1,
            )
            for k in range(OWNED)
        ],
        axis=0,
    )


def by_part(mixed):
    height = mixed.shape[0] // OWNED
    return jnp.concatenate(
        [
            jnp.concatenate(
                [
                    mixed[k * height : (k + 1) * height, r * LANES : (r + 1) * LANES]
                    for k in range(OWNED)
                ],
                axis=1,
            )
            for r in range(2)
        ],
        axis=0,
    )


def doubling():
    lane = lax.broadcasted_iota(jnp.int32, (1, OWNED * LANES), 1)
    first = lax.axis_index(IMAGE) == 0
    return jnp.where((lane < LANES) & first, 1.0, 2.0)


def started(copies, sems):
    made = [pltpu.make_async_copy(a, b, sems.at[i]) for i, (a, b) in enumerate(copies)]
    for copy in made:
        copy.start()
    return made


def forward_rows(x, u, weight, narrow, spec, hidden, slope, across, within, *scratch):
    held, near_weight, base, near, sems = scratch
    edge, local = 2 * BREADTH, pl.ds(0, LANES)
    core = lax.axis_index("core")
    copies = [
        (x.at[:, pl.ds(LANES, 2 * LANES)], held),
        (weight, near_weight),
        (narrow, base),
    ]
    for side, target in ((core, across), (1 - core, within)):
        rows = pl.multiple_of(side * (CELLS - edge), BREADTH)
        copies.append((x.at[pl.ds(rows, edge), local], target.at[pl.ds(0, edge)]))
        rows = pl.multiple_of(side * (CELLS - BREADTH), BREADTH)
        copies.append((u.at[pl.ds(rows, BREADTH), local], target.at[pl.ds(edge, BREADTH)]))
    copies = started(copies, sems)
    copies[2].wait()
    row = lax.broadcasted_iota(jnp.int32, (PEERS * OWNED * ROWS, BREADTH), 0) // 2 % HALF
    table = jnp.concatenate(
        [base[...] * (row == g).astype(F32).astype(BF) for g in range(HALF)], axis=1
    )
    copies[1].wait()
    copies[0].wait()
    pre = dot(held[...], near_weight[...])
    sigma = jax.nn.sigmoid(pre)
    low = (pre * sigma).astype(BF)
    hidden[...] = low
    for k, block in enumerate(to_owners(low, table)):
        rows = pl.ds(2 * k * ROWS, 2 * ROWS)
        near[:, rows] = block
        copies.append(pltpu.make_async_copy(near.at[:, rows], spec.at[:, rows], sems.at[7 + k]))
        if k:
            copies[-2].start()
    slope[: CELLS // 2] = slope_of(pre, sigma)[: CELLS // 2]
    copies[-1].start()
    slope[CELLS // 2 :] = slope_of(pre, sigma)[CELLS // 2 :]
    for copy in copies[3:]:
        copy.wait()


def local_part(far_x, far_u, across, within, far_weight, grad, terms, x, u, weight, sems):
    local = (slice(None), pl.ds(0, LANES))
    copies = started([(far_x.at[local], x), (far_u.at[local], u), (far_weight, weight)], sems)
    for copy in copies:
        copy.wait()
    upper = lax.axis_index("core") == 0
    above = jnp.where(upper, across[...], within[...])
    below = jnp.where(upper, within[...], across[...])
    rows = jnp.concatenate([above[: 2 * BREADTH], x[...], below[: 2 * BREADTH]], axis=0)

    def beside(cells):
        wide = cells.astype(F32)
        count = wide.shape[0]
        column = lax.broadcasted_iota(jnp.int32, wide.shape, 0) % BREADTH
        before = jnp.where(column == 0, 0.0, pltpu.roll(wide, 1, 0)).astype(BF)
        after = jnp.where(column == BREADTH - 1, 0.0, pltpu.roll(wide, count - 1, 0)).astype(BF)
        return before, after

    before, after = beside(rows)
    x3 = jnp.concatenate([before, rows, after], axis=1)
    y = jnp.zeros((CELLS + 2 * BREADTH, LANES), F32)
    for a in range(3):
        y = y + dot(
            x3[a * BREADTH : a * BREADTH + CELLS + 2 * BREADTH],
            weight[a * 3 * LANES : (a + 1) * 3 * LANES],
        )
    incoming = jnp.concatenate([above[2 * BREADTH :], u[...], below[2 * BREADTH :]], axis=0)
    d = (incoming.astype(F32) * slope_of(y, jax.nn.sigmoid(y))).astype(BF)
    before, after = beside(d)
    d3 = jnp.concatenate([after, d, before], axis=1)
    dx = u[...].astype(F32)
    for a in range(3):
        taps = [weight[(3 * a + b) * LANES : (3 * a + b + 1) * LANES] for b in range(3)]
        dx = dx + dot_t(
            d3[(2 - a) * BREADTH : (2 - a) * BREADTH + CELLS], jnp.concatenate(taps, axis=1)
        )
    grad[...] = dx.astype(BF)
    d_t = d[BREADTH : BREADTH + CELLS].T
    for a in range(3):
        found = dot(d_t, x3[(a + 1) * BREADTH : (a + 1) * BREADTH + CELLS])
        terms[a * 3 * LANES : (a + 1) * 3 * LANES] = found.T.astype(BF)
    terms[9 * LANES :] = jnp.zeros((2 * PEERS * CONV - 9 * LANES, LANES), BF)


def columns_forward(arrived, table, table_t, weight, sent, flat, slope):
    spec = by_frequency(dot(table[...], columns_of(arrived)).astype(BF))
    flat[...] = spec
    pre = dot(spec, weight[...])
    sigma = jax.nn.sigmoid(pre)
    back = dot(table_t[...], by_part((pre * sigma).astype(BF)))
    store_message(sent, blocks_of((back * doubling()).astype(BF)))
    slope[...] = slope_of(pre, sigma)


def middle_rows(arrived, hidden, u, weight, table, table_t, sent, d_combined, expand):
    spatial = from_owners(arrived[...], table_t[...])
    mix = (hidden[...].astype(F32) + spatial).astype(BF)
    y = dot(mix, weight[...])
    incoming = u[:, LANES:].astype(F32)
    d = (incoming * slope_of(y, jax.nn.sigmoid(y))).astype(BF)
    back = dot_t(d, weight[...]).astype(BF)
    d_combined[...] = back
    store_message(sent, to_owners(back, table[...]))
    found = dot(mix.T, d)
    expand[...] = jnp.concatenate([found[:, :LANES], found[:, LANES:]], axis=0).astype(BF)


def columns_backward(arrived, table, table_t, weight, slope, flat, expand, conv, sent, terms):
    found = by_frequency(dot(table[...], columns_of(arrived)) * doubling())
    d = (found * slope[...]).astype(BF)
    back = dot(table_t[...], by_part(dot_t(d, weight[...]).astype(BF)))
    store_message(sent, blocks_of(back.astype(BF)))
    spectral = dot(flat[...].T, d)
    for c in range(2):
        part = spectral[:, c * LANES : (c + 1) * LANES].reshape(PEERS, 16, LANES)
        terms[c, :, :16] = part.astype(BF)
        part = expand[c * LANES : (c + 1) * LANES].astype(F32).reshape(PEERS, 8, LANES)
        terms[c, :, 16:24] = part.astype(BF)
        part = conv[c * PEERS * CONV : (c + 1) * PEERS * CONV].astype(F32)
        terms[c, :, 24:] = part.reshape(PEERS, CONV, LANES).astype(BF)


def last_rows(arrived, d_combined, slope, x, table_t, other, d_reduce, kept, sent, terms):
    d_hidden = d_combined[...].astype(F32) + from_owners(arrived[...], table_t[...])
    d = (d_hidden * slope[...]).astype(BF)
    d_reduce[...] = d
    found = dot(d.T, x[:, LANES:]).T
    terms[...] = found.reshape(2, PEERS, 8, LANES).astype(BF)
    me = lax.axis_index("core")
    for target, core in ((kept, me), (sent, 1 - me)):
        target[:, : TERMS - 8] = other[core]
        target[:, TERMS - 8 :] = terms[core]


def added(kept, other, out):
    out[...] = (kept[...].astype(F32) + other[...].astype(F32)).astype(BF)


def global_grad(d_reduce, weight, u, local, out):
    out[:, :LANES] = local[...]
    out[:, LANES:] = (u[:, LANES:].astype(F32) + dot_t(d_reduce[...], weight[...])).astype(BF)


def summed(arrived, sent):
    total = jnp.sum(arrived[...].astype(F32), axis=0).astype(BF)
    sent[...] = jnp.broadcast_to(total[None], sent.shape)


def unpacked(factor, mine, *refs):
    results, (conv, reduce, spectral, expand), sems = refs[-9:-5], refs[-5:-1], refs[-1]
    core = lax.axis_index("core")
    core = core if len(refs) == 9 else 1 - core
    found = mine[...].astype(F32) * factor
    reduce[...] = found[:, TERMS - 8 :].reshape(LANES, LANES)
    conv[...] = found[:, 24 : 24 + CONV].reshape(PEERS * CONV, LANES)
    spectral[...] = found[:, :16].reshape(256, LANES)
    expand[...] = found[:, 16:24].reshape(LANES, LANES)
    begin = pl.multiple_of(core * LANES, LANES)
    columns = (slice(None), pl.ds(begin, LANES))
    copies = started(
        [
            (reduce, results[1].at[pl.ds(begin, LANES)]),
            (spectral, results[2].at[columns]),
            (expand, results[3].at[columns]),
        ],
        sems,
    )
    for c in range(2):
        count = min(PEERS * CONV, 9 * LANES - c * PEERS * CONV)

        @pl.when(core == c)
        def _():
            copy = pltpu.make_async_copy(
                conv.at[pl.ds(0, count)],
                results[0].at[pl.ds(c * PEERS * CONV, count)],
                sems.at[3],
            )
            copy.start()
            copy.wait()

    for copy in copies:
        copy.wait()


WHOLE = pl.BlockSpec(memory_space=pltpu.VMEM)
APART = pl.BlockSpec(memory_space=pltpu.HBM)


def placed(shape, dtype, near=True):
    return pltpu.VMEM(shape, dtype) if near else jax.ShapeDtypeStruct(shape, dtype)


def run(body, outs, *args, cost=4, specs=None, scratch=(), apart=None, aliases=None):
    many = isinstance(outs[0][0], tuple)
    return pl.pallas_call(
        body,
        out_shape=tuple(placed(*o) for o in outs) if many else placed(*outs),
        in_specs=specs or [WHOLE] * len(args),
        out_specs=tuple(APART if apart in ("all", i) else WHOLE for i in range(len(outs)))
        if many
        else WHOLE,
        input_output_aliases=aliases or {},
        scratch_shapes=scratch,
        cost_estimate=pl.CostEstimate(
            flops=int(cost * 1e8), bytes_accessed=1 << 20, transcendentals=0
        ),
        compiler_params=pltpu.CompilerParams(vmem_limit_bytes=24 << 20),
    )(*args)


def far(*arrays):
    return [pltpu.with_memory_space_constraint(a, pltpu.HBM) for a in arrays]


def other_core(array):
    return lax.ppermute(array, "core", [(0, 1), (1, 0)])


def exchange(array, axis):
    return lax.all_to_all(array, axis, 0, 0, tiled=True)


def shards(features, conv_weight, reduce_weight, spectral_weight, expand_weight, upstream):
    x = features.reshape(CELLS, 3 * LANES)
    u = upstream.reshape(CELLS, 3 * LANES)
    conv = conv_weight.reshape(9 * LANES, LANES)
    width = width_table()
    height = height_table()
    wide, wide_t = jnp.asarray(width), jnp.asarray(np.ascontiguousarray(width.T))
    tall, tall_t = jnp.asarray(height), jnp.asarray(np.ascontiguousarray(height.T))
    message = ((PEERS, OWNED * 2 * ROWS, LANES), BF)
    cells = ((CELLS, LANES), BF)
    edge = ((3 * BREADTH, LANES), BF)

    spec, hidden, slope, across, within = run(
        forward_rows,
        ((*message, False), cells, ((CELLS, LANES), F32), edge, edge),
        *far(x, u, reduce_weight, jnp.asarray(narrow_table())),
        specs=[APART] * 4,
        scratch=(
            pltpu.VMEM((CELLS, 2 * LANES), BF),
            pltpu.VMEM((2 * LANES, LANES), BF),
            pltpu.VMEM((OWNED * PEERS * ROWS, LANES), BF),
            pltpu.VMEM((PEERS, OWNED * 2 * ROWS, LANES), BF),
            pltpu.SemaphoreType.DMA((7 + OWNED,)),
        ),
        apart=0,
    )
    arrived = exchange(spec, IMAGE)
    pairs = [(i, i + 1) for i in range(1, PEERS - 1, 2)]
    across = lax.ppermute(across, IMAGE, pairs + [(b, a) for a, b in pairs])
    within = other_core(within)
    local, conv_terms = run(
        local_part,
        (cells, ((2 * PEERS * CONV, LANES), BF)),
        *(*far(x, u), across, within, *far(conv)),
        specs=[APART, APART, WHOLE, WHOLE, APART],
        scratch=(
            pltpu.VMEM((CELLS, LANES), BF),
            pltpu.VMEM((CELLS, LANES), BF),
            pltpu.VMEM((9 * LANES, LANES), BF),
            pltpu.SemaphoreType.DMA((3,)),
        ),
        cost=30,
    )
    sent, flat, mix_slope = run(
        columns_forward,
        (message, ((512, 256), BF), ((512, 256), F32)),
        *(arrived, tall, tall_t, spectral_weight),
    )
    sent, conv_terms, local = lax.optimization_barrier((sent, conv_terms, local))
    arrived = exchange(sent, IMAGE)
    sent, d_combined, expand = run(
        middle_rows,
        (message, cells, ((2 * LANES, LANES), BF)),
        *(arrived, hidden, u, expand_weight, wide, wide_t),
    )
    arrived = exchange(sent, IMAGE)
    sent, other = run(
        columns_backward,
        (message, ((2, PEERS, TERMS - 8, LANES), BF)),
        *(arrived, tall, tall_t, spectral_weight, mix_slope, flat, expand, conv_terms),
    )
    arrived = exchange(sent, IMAGE)
    packed = ((PEERS, TERMS, LANES), BF)
    d_reduce, kept, sent = run(
        last_rows,
        (cells, packed, packed),
        *(arrived, d_combined, slope, x, wide_t, other),
        scratch=(pltpu.VMEM((2, PEERS, 8, LANES), BF),),
    )
    arrived = other_core(sent)
    grad = run(
        global_grad, ((CELLS, 3 * LANES), BF, False), *(d_reduce, reduce_weight, u, local), cost=10
    )
    sums, grad = lax.optimization_barrier((run(added, packed, kept, arrived), grad))
    arrived = exchange(sums, DP)
    sums = run(summed, ((LEVELS, TERMS, LANES), BF), arrived)
    arrived = exchange(sums, "z")
    sums = run(summed, packed, arrived)
    arrived = exchange(sums, DP)
    factor = 1.0 / math.sqrt(PEERS * PEERS * ROWS * BREADTH)
    halves = dict(
        outs=(
            ((9 * LANES, LANES), F32, False),
            ((256, LANES), F32, False),
            ((256, 256), F32, False),
            ((128, 256), F32, False),
        ),
        scratch=(
            pltpu.VMEM((PEERS * CONV, LANES), F32),
            pltpu.VMEM((LANES, LANES), F32),
            pltpu.VMEM((256, LANES), F32),
            pltpu.VMEM((LANES, LANES), F32),
            pltpu.SemaphoreType.DMA((4,)),
        ),
        apart="all",
    )
    unpack = functools.partial(unpacked, factor)
    own = run(unpack, halves.pop("outs"), arrived, cost=10, **halves)
    conv_sum, reduce_sum, spectral_sum, expand_sum = run(
        unpack,
        tuple((a.shape, a.dtype, False) for a in own),
        *(other_core(arrived), *own),
        specs=[WHOLE, *(APART,) * 4],
        aliases={i + 1: i for i in range(4)},
        **halves,
    )
    return (
        grad.reshape(1, ROWS, BREADTH, 3 * LANES),
        conv_sum.reshape(3, 3, LANES, LANES),
        reduce_sum,
        spectral_sum,
        expand_sum,
    )


def solution(mesh):
    strips = P(DP, IMAGE, None, None)
    return jax.shard_map(
        shards,
        mesh=Mesh(mesh.devices.reshape(LEVELS, 2, SIDE, SIDE), (*IMAGE, *DP)),
        in_specs=(strips, P(), P(), P(), P(), strips),
        out_specs=(strips, P(), P(), P(), P()),
        check_vma=False,
    )
```

```python
import functools
import math

import jax
import jax.numpy as jnp
import numpy as np
from jax import lax
from jax.experimental import pallas as pl
from jax.experimental.pallas import tpu as pltpu
from jax.sharding import PartitionSpec as P

BF = jnp.bfloat16
F32 = jnp.float32
PEERS = 16
ROWS = 8
BREADTH = 128
CELLS = ROWS * BREADTH
LANES = 128
OWNED = 4
HALF = ROWS // 2
LEVELS = 8
STRIPS = tuple(2 * z + core for z in (4, 3, 2, 1, 0, 7, 6, 5) for core in (1, 0))
COLUMNS = tuple(tuple(s for s in STRIPS if s % 2 == core) for core in range(2))
IMAGES = tuple((y + 2) % 4 * 4 + (x + 2) % 4 for y in range(4) for x in range(4))
CONV = 40
TERMS = 16 + 8 + CONV + 8


def width_table():
    w = np.arange(BREADTH)
    freq = np.arange(PEERS * OWNED).reshape(PEERS, OWNED)
    phase = (w[None, None, :] * freq[:, :, None] % BREADTH) * (2.0 * math.pi / BREADTH)
    factor = 1.0 / math.sqrt(BREADTH)
    base = np.stack([np.cos(phase) * factor, -np.sin(phase) * factor], axis=2)
    table = np.einsum("jkrw,hg->kjhrgw", base, np.eye(HALF))
    return table.reshape(OWNED * PEERS * HALF * 2, HALF * BREADTH).astype(BF)


def narrow_table():
    table = width_table().reshape(OWNED, PEERS, HALF, 2, HALF, BREADTH)
    return np.einsum("kjhrhw->kjhrw", table).reshape(-1, BREADTH)


def height_table():
    height = PEERS * ROWS
    h = np.arange(height)
    rows = h.reshape(PEERS, ROWS)[list(STRIPS)].reshape(height)
    phase = (rows[:, None] * h[None, :] % height) * (2.0 * math.pi / height)
    factor = 1.0 / math.sqrt(height)
    cosine, sine = np.cos(phase) * factor, -np.sin(phase) * factor
    table = np.zeros((2, height, height, 2))
    table[0, :, :, 0] = cosine.T
    table[0, :, :, 1] = -sine.T
    table[1, :, :, 1] = cosine.T
    table[1, :, :, 0] = sine.T
    return table.reshape(2 * height, 2 * height).astype(BF)


def dot(left, right):
    return jnp.dot(left, right, preferred_element_type=F32)


def dot_t(left, right):
    return lax.dot_general(left, right, (((1,), (1,)), ((), ())), preferred_element_type=F32)


def slope_of(values, sigma):
    return sigma * (1.0 + values * (1.0 - sigma))


def to_owners(cells, table):
    side = jnp.concatenate([cells[: CELLS // 2], cells[CELLS // 2 :]], axis=1)
    found = dot(table, side)
    parts = [
        found[:, q * LANES : (q + 1) * LANES].reshape(OWNED, PEERS, ROWS, LANES) for q in range(2)
    ]
    joined = jnp.concatenate(parts, axis=2).astype(BF)
    return [joined[k] for k in range(OWNED)]


def from_owners(strip, table_t):
    wide = strip.astype(F32)
    halves = []
    for q in range(2):
        rows = [
            wide[:, (2 * k + q) * ROWS : (2 * k + q + 1) * ROWS].reshape(PEERS * ROWS, LANES)
            for k in range(OWNED)
        ]
        halves.append(jnp.concatenate(rows, axis=0).astype(BF))
    found = dot(table_t, jnp.concatenate(halves, axis=1))
    return jnp.concatenate([found[:, :LANES], found[:, LANES:]], axis=0)


def store_message(sent, blocks):
    for k, block in enumerate(blocks):
        sent[:, 2 * k * ROWS : 2 * (k + 1) * ROWS] = block


def columns_of(arrived):
    return jnp.concatenate(
        [
            arrived[:, 2 * k * ROWS : 2 * (k + 1) * ROWS].reshape(PEERS * ROWS * 2, LANES)
            for k in range(OWNED)
        ],
        axis=1,
    )


def blocks_of(columns):
    return [
        columns[:, k * LANES : (k + 1) * LANES].reshape(PEERS, 2 * ROWS, LANES)
        for k in range(OWNED)
    ]


def by_frequency(columns):
    height = columns.shape[0] // 2
    return jnp.concatenate(
        [
            jnp.concatenate(
                [
                    columns[:height, k * LANES : (k + 1) * LANES],
                    columns[height:, k * LANES : (k + 1) * LANES],
                ],
                axis=1,
            )
            for k in range(OWNED)
        ],
        axis=0,
    )


def by_part(mixed):
    height = mixed.shape[0] // OWNED
    return jnp.concatenate(
        [
            jnp.concatenate(
                [
                    mixed[k * height : (k + 1) * height, r * LANES : (r + 1) * LANES]
                    for k in range(OWNED)
                ],
                axis=1,
            )
            for r in range(2)
        ],
        axis=0,
    )


def core_index():
    return lax.rem(lax.axis_index("image"), 2)


def doubling():
    lane = lax.broadcasted_iota(jnp.int32, (1, OWNED * LANES), 1)
    first = lax.axis_index("image") == STRIPS[0]
    return jnp.where((lane < LANES) & first, 1.0, 2.0)


def started(copies, sems):
    made = [pltpu.make_async_copy(a, b, sems.at[i]) for i, (a, b) in enumerate(copies)]
    for copy in made:
        copy.start()
    return made


def forward_rows(x, u, weight, narrow, spec, hidden, slope, across, within, *scratch):
    held, near_weight, base, near, sems = scratch
    edge, local = 2 * BREADTH, pl.ds(0, LANES)
    core = core_index()
    copies = [
        (narrow, base),
        (weight, near_weight),
        (x.at[:, pl.ds(LANES, 2 * LANES)], held),
    ]
    for side, target in ((core, across), (1 - core, within)):
        rows = pl.multiple_of(side * (CELLS - edge), BREADTH)
        copies.append((x.at[pl.ds(rows, edge), local], target.at[pl.ds(0, edge)]))
        rows = pl.multiple_of(side * (CELLS - BREADTH), BREADTH)
        copies.append((u.at[pl.ds(rows, BREADTH), local], target.at[pl.ds(edge, BREADTH)]))
    copies = started(copies, sems)
    copies[0].wait()
    row = lax.broadcasted_iota(jnp.int32, (PEERS * OWNED * ROWS, BREADTH), 0) // 2 % HALF
    table = jnp.concatenate(
        [base[...] * (row == g).astype(F32).astype(BF) for g in range(HALF)], axis=1
    )
    copies[1].wait()
    copies[2].wait()
    pre = dot(held[...], near_weight[...])
    sigma = jax.nn.sigmoid(pre)
    low = (pre * sigma).astype(BF)
    hidden[...] = low
    for k, block in enumerate(to_owners(low, table)):
        rows = pl.ds(2 * k * ROWS, 2 * ROWS)
        near[:, rows] = block
        copies.append(pltpu.make_async_copy(near.at[:, rows], spec.at[:, rows], sems.at[7 + k]))
        if k:
            copies[-2].start()
    slope[: CELLS // 2] = slope_of(pre, sigma)[: CELLS // 2]
    copies[-1].start()
    slope[CELLS // 2 :] = slope_of(pre, sigma)[CELLS // 2 :]
    for copy in copies[3:]:
        copy.wait()


def local_part(far_x, far_u, across, within, far_weight, grad, terms, x, u, weight, sems):
    local = (slice(None), pl.ds(0, LANES))
    copies = started([(far_x.at[local], x), (far_u.at[local], u), (far_weight, weight)], sems)
    for copy in copies:
        copy.wait()
    upper = core_index() == 0
    above = jnp.where(upper, across[...], within[...])
    below = jnp.where(upper, within[...], across[...])
    rows = jnp.concatenate([above[: 2 * BREADTH], x[...], below[: 2 * BREADTH]], axis=0)

    def beside(cells):
        wide = cells.astype(F32)
        count = wide.shape[0]
        column = lax.broadcasted_iota(jnp.int32, wide.shape, 0) % BREADTH
        before = jnp.where(column == 0, 0.0, pltpu.roll(wide, 1, 0)).astype(BF)
        after = jnp.where(column == BREADTH - 1, 0.0, pltpu.roll(wide, count - 1, 0)).astype(BF)
        return before, after

    before, after = beside(rows)
    x3 = jnp.concatenate([before, rows, after], axis=1)
    y = jnp.zeros((CELLS + 2 * BREADTH, LANES), F32)
    for a in range(3):
        y = y + dot(
            x3[a * BREADTH : a * BREADTH + CELLS + 2 * BREADTH],
            weight[a * 3 * LANES : (a + 1) * 3 * LANES],
        )
    incoming = jnp.concatenate([above[2 * BREADTH :], u[...], below[2 * BREADTH :]], axis=0)
    d = (incoming.astype(F32) * slope_of(y, jax.nn.sigmoid(y))).astype(BF)
    before, after = beside(d)
    d3 = jnp.concatenate([after, d, before], axis=1)
    dx = u[...].astype(F32)
    for a in range(3):
        taps = [weight[(3 * a + b) * LANES : (3 * a + b + 1) * LANES] for b in range(3)]
        dx = dx + dot_t(
            d3[(2 - a) * BREADTH : (2 - a) * BREADTH + CELLS], jnp.concatenate(taps, axis=1)
        )
    grad[...] = dx.astype(BF)
    d_t = d[BREADTH : BREADTH + CELLS].T
    for a in range(3):
        found = dot(d_t, x3[(a + 1) * BREADTH : (a + 1) * BREADTH + CELLS])
        terms[a * 3 * LANES : (a + 1) * 3 * LANES] = found.T.astype(BF)
    terms[9 * LANES :] = jnp.zeros((2 * PEERS * CONV - 9 * LANES, LANES), BF)


def columns_forward(arrived, table, table_t, weight, sent, flat, slope):
    spec = by_frequency(dot(table[...], columns_of(arrived)).astype(BF))
    flat[...] = spec
    pre = dot(spec, weight[...])
    sigma = jax.nn.sigmoid(pre)
    back = dot(table_t[...], by_part((pre * sigma).astype(BF)))
    store_message(sent, blocks_of((back * doubling()).astype(BF)))
    slope[...] = slope_of(pre, sigma)


def middle_rows(arrived, hidden, u, weight, table, table_t, sent, d_combined, expand):
    spatial = from_owners(arrived[...], table_t[...])
    mix = (hidden[...].astype(F32) + spatial).astype(BF)
    y = dot(mix, weight[...])
    incoming = u[:, LANES:].astype(F32)
    d = (incoming * slope_of(y, jax.nn.sigmoid(y))).astype(BF)
    back = dot_t(d, weight[...]).astype(BF)
    d_combined[...] = back
    store_message(sent, to_owners(back, table[...]))
    found = dot(mix.T, d)
    expand[...] = jnp.concatenate([found[:, :LANES], found[:, LANES:]], axis=0).astype(BF)


def columns_backward(arrived, table, table_t, weight, slope, flat, expand, conv, sent, terms):
    found = by_frequency(dot(table[...], columns_of(arrived)) * doubling())
    d = (found * slope[...]).astype(BF)
    back = dot(table_t[...], by_part(dot_t(d, weight[...]).astype(BF)))
    store_message(sent, blocks_of(back.astype(BF)))
    spectral = dot(flat[...].T, d)
    for c in range(2):
        part = spectral[:, c * LANES : (c + 1) * LANES].reshape(PEERS, 16, LANES)
        terms[c, :, :16] = part.astype(BF)
        part = expand[c * LANES : (c + 1) * LANES].astype(F32).reshape(PEERS, 8, LANES)
        terms[c, :, 16:24] = part.astype(BF)
        part = conv[c * PEERS * CONV : (c + 1) * PEERS * CONV].astype(F32)
        terms[c, :, 24:] = part.reshape(PEERS, CONV, LANES).astype(BF)


def last_rows(arrived, d_combined, slope, x, table_t, other, d_reduce, kept, sent, terms):
    d_hidden = d_combined[...].astype(F32) + from_owners(arrived[...], table_t[...])
    d = (d_hidden * slope[...]).astype(BF)
    d_reduce[...] = d
    found = dot(d.T, x[:, LANES:]).T
    terms[...] = found.reshape(2, PEERS, 8, LANES).astype(BF)
    me = core_index()
    for target, core in ((kept, me), (sent, 1 - me)):
        target[:, : TERMS - 8] = other[core]
        target[:, TERMS - 8 :] = terms[core]


def added(kept, other, out):
    out[...] = (kept[...].astype(F32) + other[...].astype(F32)).astype(BF)


def global_grad(d_reduce, weight, u, local, out):
    out[:, :LANES] = local[...]
    out[:, LANES:] = (u[:, LANES:].astype(F32) + dot_t(d_reduce[...], weight[...])).astype(BF)


def summed(arrived, sent):
    total = jnp.sum(arrived[...].astype(F32), axis=0).astype(BF)
    sent[...] = jnp.broadcast_to(total[None], sent.shape)


def unpacked(factor, mine, *refs):
    results, (conv, reduce, spectral, expand), sems = refs[-9:-5], refs[-5:-1], refs[-1]
    core = core_index()
    core = core if len(refs) == 9 else 1 - core
    found = mine[...].astype(F32) * factor
    reduce[...] = found[:, TERMS - 8 :].reshape(LANES, LANES)
    conv[...] = found[:, 24 : 24 + CONV].reshape(PEERS * CONV, LANES)
    spectral[...] = found[:, :16].reshape(256, LANES)
    expand[...] = found[:, 16:24].reshape(LANES, LANES)
    begin = pl.multiple_of(core * LANES, LANES)
    columns = (slice(None), pl.ds(begin, LANES))
    copies = started(
        [
            (reduce, results[1].at[pl.ds(begin, LANES)]),
            (spectral, results[2].at[columns]),
            (expand, results[3].at[columns]),
        ],
        sems,
    )
    for c in range(2):
        count = min(PEERS * CONV, 9 * LANES - c * PEERS * CONV)

        @pl.when(core == c)
        def _():
            copy = pltpu.make_async_copy(
                conv.at[pl.ds(0, count)],
                results[0].at[pl.ds(c * PEERS * CONV, count)],
                sems.at[3],
            )
            copy.start()
            copy.wait()

    for copy in copies:
        copy.wait()


WHOLE = pl.BlockSpec(memory_space=pltpu.VMEM)
APART = pl.BlockSpec(memory_space=pltpu.HBM)


def placed(shape, dtype, near=True):
    return pltpu.VMEM(shape, dtype) if near else jax.ShapeDtypeStruct(shape, dtype)


def run(body, outs, *args, cost=4, specs=None, scratch=(), apart=None, aliases=None):
    many = isinstance(outs[0][0], tuple)
    return pl.pallas_call(
        body,
        out_shape=tuple(placed(*o) for o in outs) if many else placed(*outs),
        in_specs=specs or [WHOLE] * len(args),
        out_specs=tuple(APART if apart in ("all", i) else WHOLE for i in range(len(outs)))
        if many
        else WHOLE,
        input_output_aliases=aliases or {},
        scratch_shapes=scratch,
        cost_estimate=pl.CostEstimate(
            flops=int(cost * 1e8), bytes_accessed=1 << 20, transcendentals=0
        ),
        compiler_params=pltpu.CompilerParams(vmem_limit_bytes=24 << 20),
    )(*args)


def far(*arrays):
    return [pltpu.with_memory_space_constraint(a, pltpu.HBM) for a in arrays]


def other_core(array):
    return lax.ppermute(array, "image", [(i, i ^ 1) for i in range(PEERS)])


def exchange(array, axis, *groups):
    return lax.all_to_all(array, axis, 0, 0, tiled=True, axis_index_groups=groups)


def shards(features, conv_weight, reduce_weight, spectral_weight, expand_weight, upstream):
    x = features.reshape(CELLS, 3 * LANES)
    u = upstream.reshape(CELLS, 3 * LANES)
    conv = conv_weight.reshape(9 * LANES, LANES)
    width = width_table()
    height = height_table()
    wide, wide_t = jnp.asarray(width), jnp.asarray(np.ascontiguousarray(width.T))
    tall, tall_t = jnp.asarray(height), jnp.asarray(np.ascontiguousarray(height.T))
    message = ((PEERS, OWNED * 2 * ROWS, LANES), BF)
    cells = ((CELLS, LANES), BF)
    edge = ((3 * BREADTH, LANES), BF)

    spec, hidden, slope, across, within = run(
        forward_rows,
        ((*message, False), cells, ((CELLS, LANES), F32), edge, edge),
        *far(x, u, reduce_weight, jnp.asarray(narrow_table())),
        specs=[APART] * 4,
        scratch=(
            pltpu.VMEM((CELLS, 2 * LANES), BF),
            pltpu.VMEM((2 * LANES, LANES), BF),
            pltpu.VMEM((OWNED * PEERS * ROWS, LANES), BF),
            pltpu.VMEM((PEERS, OWNED * 2 * ROWS, LANES), BF),
            pltpu.SemaphoreType.DMA((7 + OWNED,)),
        ),
        apart=0,
    )
    arrived = exchange(spec, "image", STRIPS)
    pairs = [(i, i + 1) for i in range(1, PEERS - 1, 2)]
    across = lax.ppermute(across, "image", pairs + [(b, a) for a, b in pairs])
    within = other_core(within)
    local, conv_terms = run(
        local_part,
        (cells, ((2 * PEERS * CONV, LANES), BF)),
        *(*far(x, u), across, within, *far(conv)),
        specs=[APART, APART, WHOLE, WHOLE, APART],
        scratch=(
            pltpu.VMEM((CELLS, LANES), BF),
            pltpu.VMEM((CELLS, LANES), BF),
            pltpu.VMEM((9 * LANES, LANES), BF),
            pltpu.SemaphoreType.DMA((3,)),
        ),
        cost=30,
    )
    sent, flat, mix_slope = run(
        columns_forward,
        (message, ((512, 256), BF), ((512, 256), F32)),
        *(arrived, tall, tall_t, spectral_weight),
    )
    sent, conv_terms, local = lax.optimization_barrier((sent, conv_terms, local))
    arrived = exchange(sent, "image", STRIPS)
    sent, d_combined, expand = run(
        middle_rows,
        (message, cells, ((2 * LANES, LANES), BF)),
        *(arrived, hidden, u, expand_weight, wide, wide_t),
    )
    arrived = exchange(sent, "image", STRIPS)
    sent, other = run(
        columns_backward,
        (message, ((2, PEERS, TERMS - 8, LANES), BF)),
        *(arrived, tall, tall_t, spectral_weight, mix_slope, flat, expand, conv_terms),
    )
    arrived = exchange(sent, "image", STRIPS)
    packed = ((PEERS, TERMS, LANES), BF)
    d_reduce, kept, sent = run(
        last_rows,
        (cells, packed, packed),
        *(arrived, d_combined, slope, x, wide_t, other),
        scratch=(pltpu.VMEM((2, PEERS, 8, LANES), BF),),
    )
    arrived = other_core(sent)
    grad = run(
        global_grad, ((CELLS, 3 * LANES), BF, False), *(d_reduce, reduce_weight, u, local), cost=10
    )
    sums, grad = lax.optimization_barrier((run(added, packed, kept, arrived), grad))
    arrived = exchange(sums, "dp", IMAGES)
    sums = run(summed, ((LEVELS, TERMS, LANES), BF), arrived)
    arrived = exchange(sums, "image", *COLUMNS)
    sums = run(summed, packed, arrived)
    arrived = exchange(sums, "dp", IMAGES)
    factor = 1.0 / math.sqrt(PEERS * PEERS * ROWS * BREADTH)
    halves = dict(
        outs=(
            ((9 * LANES, LANES), F32, False),
            ((256, LANES), F32, False),
            ((256, 256), F32, False),
            ((128, 256), F32, False),
        ),
        scratch=(
            pltpu.VMEM((PEERS * CONV, LANES), F32),
            pltpu.VMEM((LANES, LANES), F32),
            pltpu.VMEM((256, LANES), F32),
            pltpu.VMEM((LANES, LANES), F32),
            pltpu.SemaphoreType.DMA((4,)),
        ),
        apart="all",
    )
    unpack = functools.partial(unpacked, factor)
    own = run(unpack, halves.pop("outs"), arrived, cost=10, **halves)
    conv_sum, reduce_sum, spectral_sum, expand_sum = run(
        unpack,
        tuple((a.shape, a.dtype, False) for a in own),
        *(other_core(arrived), *own),
        specs=[WHOLE, *(APART,) * 4],
        aliases={i + 1: i for i in range(4)},
        **halves,
    )
    return (
        grad.reshape(1, ROWS, BREADTH, 3 * LANES),
        conv_sum.reshape(3, 3, LANES, LANES),
        reduce_sum,
        spectral_sum,
        expand_sum,
    )


def solution(mesh):
    strips = P("dp", "image", None, None)
    return jax.shard_map(
        shards,
        mesh=mesh,
        in_specs=(strips, P(), P(), P(), P(), strips),
        out_specs=(strips, P(), P(), P(), P()),
        check_vma=False,
    )
```
